32 devices in a mesh: layer: 8 (over z, x), rep: 4 (over y, core).
Axes of the slice: x: 2, y: 2, z: 4, core: 2. Of those that a mesh axis runs over, the one named last changes fastest.
Arguments:
- inverse_root: bfloat16 [64, 16, 128, 128], P('layer', 'rep'), may hold values from -0.625 to 0.625
- square_root: bfloat16 [64, 16, 128, 128], P('layer', 'rep'), may hold values from -0.625 to 0.625
- pattern: int32 [64, 16], P('layer', 'rep'), may hold values from 0 to 1, as said below
Outputs:
- inverse_next: bfloat16 [64, 16, 128, 128], P('layer', 'rep')
- square_next: bfloat16 [64, 16, 128, 128], P('layer', 'rep')
The draws below stay inside these ranges and needn't reach their ends.
Inputs may be any that keep to these rules, and one draw needn't show every extreme that they name: 1 marks a tile of the common pattern. Slot 8 is 1 in every block row, and slot w of block row i is 0 where i - 8 + w lies outside 0 to 63.
All inputs are finite; a program needn't handle non-finite values.
Results may differ from the reference program's by a relative error of at most 0.018.
Values may be sent and summed in bfloat16 or wider, within the bound.
A program may use at most 128 MiB of HBM per device.

```python
import jax
import jax.numpy as jnp
from jax import lax

TILE = 128
BAND = 16
HALF = 8
NB = 64
N_REP = 4


def draw_pattern(key, part):
    row_ids = jnp.arange(NB, dtype=jnp.int32)[:, None]
    slot_ids = jnp.arange(BAND, dtype=jnp.int32)[None, :]
    column = row_ids - HALF + slot_ids
    inside = (column >= 0) & (column < NB)
    key_level = jax.random.fold_in(key, 11)
    key_tiles = jax.random.fold_in(key, 23)
    fill_level = jax.random.randint(key_level, (NB, 1), 15, 90)
    tile_draws = jax.random.randint(key_tiles, (NB, BAND), 0, 100)
    chosen = (tile_draws < fill_level) | (slot_ids == HALF)
    return (inside & chosen).astype(jnp.int32)


def shard_levels(own_key, shape, shards, low, high):
    def one(position, shards_of):
        draws = jax.random.uniform(jax.random.fold_in(jax.random.fold_in(own_key, 6), position), (shards_of,), jnp.float32, low / len(shards), high / len(shards))
        return jnp.repeat(jnp.exp(draws), shape[position] // shards_of).reshape((-1,) + (1,) * (len(shape) - position - 1))

    level = one(*shards[0])
    for cut in shards[1:]:
        level = level * one(*cut)
    return level


def bell_draw(rng, shape, width, bound, pieces=(), kind=jnp.bfloat16):
    factor_of = shard_levels(rng, shape, pieces, -0.22, 0.18) if pieces else 1.0
    drawn = jax.random.normal(rng, shape, jnp.float32) * width * factor_of
    return jnp.minimum(jnp.maximum(drawn, -bound), bound).astype(kind)


def setup_inputs(seed: int = 0) -> dict:
    streams_of = jax.random.split(jax.random.key(seed), 4)
    return {
        "inverse_root": bell_draw(streams_of[0], (NB, BAND, TILE, TILE), 0.1, 0.625, ((0, 8), (1, 4))),
        "square_root": bell_draw(streams_of[1], (NB, BAND, TILE, TILE), 0.1, 0.625, ((0, 8), (1, 4))),
        "pattern": draw_pattern(jax.random.fold_in(streams_of[3], 71), 0),
    }


def band_product(left_tiles, right_tiles):
    block_rows = left_tiles.shape[0]
    band_slots = left_tiles.shape[1]
    half_band = band_slots // 2
    group_slots = band_slots // N_REP
    padded = jnp.pad(right_tiles, ((half_band, half_band), (band_slots, band_slots), (0, 0), (0, 0)))
    total = jnp.zeros(left_tiles.shape, jnp.float32)
    for group in range(N_REP):
        partial_value = jnp.zeros(left_tiles.shape, jnp.float32)
        for inner in range(group * group_slots, (group + 1) * group_slots):
            low_slot = max(0, inner - half_band)
            high_slot = min(band_slots, inner + half_band)
            offset = band_slots + half_band - inner
            shifted = padded[inner:inner + block_rows, offset + low_slot:offset + high_slot]
            product = jnp.einsum("iab,iwbc->iwac", left_tiles[:, inner].astype(jnp.float32), shifted.astype(jnp.float32))
            partial_value = partial_value.at[:, low_slot:high_slot].add(product)
        rounded = lax.optimization_barrier(partial_value.astype(jnp.bfloat16))
        total = total + rounded.astype(jnp.float32)
    return total


def reference(inverse_root, square_root, pattern):
    in_pattern = (pattern == 1)[:, :, None, None]
    inverse_kept = jnp.where(in_pattern, inverse_root, jnp.zeros_like(inverse_root))
    square_kept = jnp.where(in_pattern, square_root, jnp.zeros_like(square_root))
    intersection = jnp.where(in_pattern, band_product(inverse_kept, square_kept), jnp.float32(0.0))
    band_slots = pattern.shape[1]
    half_band = band_slots // 2
    diagonal = (jnp.arange(band_slots, dtype=jnp.int32) == half_band).astype(jnp.float32)
    identity = jnp.eye(inverse_root.shape[2], dtype=jnp.float32)
    update = jnp.where(in_pattern, 1.5 * diagonal[None, :, None, None] * identity - 0.5 * intersection, jnp.float32(0.0)).astype(jnp.bfloat16)
    square_next = jnp.where(in_pattern, band_product(square_kept, update), jnp.float32(0.0)).astype(jnp.bfloat16)
    inverse_next = jnp.where(in_pattern, band_product(update, inverse_kept), jnp.float32(0.0)).astype(jnp.bfloat16)
    return inverse_next, square_next
```

```python
import functools

import jax
import jax.numpy as jnp
from jax import lax
from jax.experimental import pallas as pl
from jax.experimental.pallas import tpu as pltpu
from jax.sharding import PartitionSpec as P

MESH = pl.DeviceIdType.MESH
VMEM = pl.BlockSpec(memory_space=pltpu.VMEM)
SMEM = pl.BlockSpec(memory_space=pltpu.SMEM)
SEMAPHORES = 256


def reached(rows, band, low, high):
    half = band // 2
    found = {1: {}, -1: {}}
    for i in range(rows):
        for u in range(band):
            j = i - half + u
            if 0 <= j < rows:
                continue
            assert -rows <= j < 2 * rows
            side, a = (1, j + rows) if j < 0 else (-1, j - rows)
            for w in range(low, high):
                v = w + half - u
                if 0 <= v < band:
                    lo, hi = found[side].get(a, (v, v + 1))
                    found[side][a] = (min(lo, v), max(hi, v + 1))
    return found


def rectangles(spans, first, last):
    cut = []
    for a in sorted(spans):
        lo, hi = max(spans[a][0], first), min(spans[a][1], last)
        if lo >= hi:
            continue
        if cut and cut[-1][1] == a and cut[-1][2:] == (lo, hi):
            cut[-1] = (cut[-1][0], a + 1, lo, hi)
        else:
            cut.append((a, a + 1, lo, hi))
    return cut


class Later:
    def __init__(self, make, args=None):
        self.make, self.args = make, args

    def __call__(self, *args):
        return Later(self.make, args)

    def start(self):
        self.make(*self.args).start()

    def wait_recv(self):
        self.make(*self.args).wait_recv()

    def wait_send(self):
        self.make(*self.args).wait_send()


def step_kernel(layers, reps, refs_shape, pattern, z_own, y_own, z_next, y_next, y_wide, z_wide, u_wide, send_sems, recv_sems):
    rows, slots, tile = refs_shape
    band = slots * reps
    half = band // 2
    layer, rep = lax.axis_index("layer"), lax.axis_index("rep")
    after, before = lax.rem(layer + 1, layers), lax.rem(layer + layers - 1, layers)
    may_send = {1: layer + 1 < layers, -1: layer > 0}
    may_take = {1: layer > 0, -1: layer + 1 < layers}
    bits = []
    bit = reps // 2
    while bit >= 2:
        bits.append(bit)
        bit //= 2
    masks = list(range(0, reps, 2))
    keys = {}
    wides = {"y": y_wide, "z": z_wide, "u": u_wide}
    relayed = ("z", "u") if reps == 4 else ()

    def keep(i, _):
        for w in range(slots):
            good = pattern[i, w] == 1
            for own, wide in ((y_own, y_wide), (z_own, z_wide)):
                part = own[i, w]
                wide[rows + i, rep * slots + w] = jnp.where(good, part, jnp.zeros_like(part))
        return 0

    lax.fori_loop(0, rows, keep, 0)

    barrier = pltpu.get_barrier_semaphore()
    for place in (after, before):
        pl.semaphore_signal(barrier, inc=1, device_id={"layer": place}, device_id_type=MESH)
    for flip in [1] + bits:
        partner = rep + flip * (1 - 2 * lax.rem(lax.div(rep, flip), 2))
        pl.semaphore_signal(barrier, inc=1, device_id={"rep": partner}, device_id_type=MESH)
    pl.semaphore_wait(barrier, 3 + len(bits))

    def schedule(me):
        chip = me // 2
        remote = []
        need = reached(rows, band, chip * 2 * slots, (chip + 1) * 2 * slots)
        union = reached(rows, band, 0, band)
        other = reached(rows, band, (1 - chip) * 2 * slots, (2 - chip) * 2 * slots) if relayed else None
        direct_side = 1 if chip == 0 else -1

        def spans(s, side):
            if s not in relayed:
                return need[side]
            return union[side] if side == direct_side else {}

        def arriving(s, side):
            return spans(s, side) or need[side]

        def cut(which, q):
            return rectangles(which, q * slots, (q + 1) * slots)

        def base(side):
            return 0 if side == 1 else 2 * rows

        def copy(key, src, dst, device):
            n = keys.setdefault(key, len(keys))
            return pltpu.make_async_remote_copy(
                src_ref=src, dst_ref=dst, send_sem=send_sems.at[n], recv_sem=recv_sems.at[n],
                device_id=device, device_id_type=MESH,
            )

        def begin(guard, made):
            remote.append((guard, made))
            if guard is None:
                made.start()
            else:
                pl.when(guard)(made.start)

        def shard(s, q):
            return wides[s].at[pl.ds(rows, rows), pl.ds(q * slots, slots)]

        @Later
        def across(s, m, bit):
            part = shard(s, me ^ bit ^ m)
            return copy(("y", s, m), part, part, {"rep": me ^ bit})

        @Later
        def across_in(s, m, bit):
            part = shard(s, me ^ m)
            return copy(("y", s, m), part, part, {"rep": me ^ bit})

        @Later
        def to_core(s, m):
            part = shard(s, me ^ m)
            return copy(("d", s, m), part, part, {"rep": me ^ 1})

        @Later
        def to_core_in(s, m):
            part = shard(s, me ^ 1 ^ m)
            return copy(("d", s, m), part, part, {"rep": me ^ 1})

        @Later
        def to_layer(s, side, m, k, piece):
            a, b, lo, hi = piece
            src = wides[s].at[pl.ds(rows + a, b - a), pl.ds(lo, hi - lo)]
            dst = wides[s].at[pl.ds(base(side) + a, b - a), pl.ds(lo, hi - lo)]
            return copy(("x", s, side, m, k), src, dst, {"layer": after if side == 1 else before})

        @Later
        def relay(s, side, m, k, piece):
            a, b, lo, hi = piece
            part = wides[s].at[pl.ds(base(side) + a, b - a), pl.ds(lo, hi - lo)]
            return copy(("r", s, side, m, k), part, part, {"rep": me ^ 2})

        @Later
        def halo_to_core(s, side, m, q):
            pieces = cut(arriving(s, side), q)
            a, b = min(c[0] for c in pieces), max(c[1] for c in pieces)
            part = wides[s].at[pl.ds(base(side) + a, b - a), pl.ds(q * slots, slots)]
            return copy(("h", s, side, m), part, part, {"rep": me ^ 1})

        def send_layer(s, m):
            for side in (1, -1):
                for k, piece in enumerate(cut(spans(s, side), me ^ m)):
                    begin(may_send[side], to_layer(s, side, m, k, piece))

        def take_direct(s, m):
            for side in (1, -1):
                pieces = cut(spans(s, side), me ^ m)
                if pieces:
                    made = [to_layer(s, side, m, k, piece) for k, piece in enumerate(pieces)]
                    onward = [halo_to_core(s, side, m, me ^ m)]
                    if s in relayed:
                        onward += [
                            relay(s, side, m ^ 2, k, piece)
                            for k, piece in enumerate(cut(other[side], me ^ m))
                        ]
                    pass_on(side, made, onward)

        def take_relayed(s, m):
            for side in (1, -1):
                if s in relayed and side != direct_side:
                    pieces = cut(need[side], me ^ m)
                    if pieces:
                        made = [relay(s, side, m, k, piece) for k, piece in enumerate(pieces)]
                        pass_on(side, made, [halo_to_core(s, side, m, me ^ m)])

        def pass_on(side, made, onward):
            remote.extend((may_take[side], o) for o in onward)

            @pl.when(may_take[side])
            def _():
                for one in made:
                    one.wait_recv()
                for one in onward:
                    one.start()

        def start_gather(s):
            if bits:
                begin(None, across(s, bits[0], bits[0]))
            begin(None, to_core(s, 0))

        def gather(s, halo):
            held = [0]
            for n, bit in enumerate(bits):
                if n > 0:
                    for m in held:
                        begin(None, across(s, m ^ bit, bit))
                fresh = [m ^ bit for m in held]
                for m in fresh:
                    across_in(s, m, bit).wait_recv()
                    begin(None, to_core(s, m))
                    if halo:
                        send_layer(s, m)
                held = held + fresh

        def finish_own(s):
            for m in masks:
                to_core_in(s, m).wait_recv()

        def finish_halo(s):
            for side in (1, -1):
                made = [
                    halo_to_core(s, side, m, me ^ 1 ^ m)
                    for m in masks
                    if cut(arriving(s, side), me ^ 1 ^ m)
                ]

                @pl.when(may_take[side])
                def _():
                    for one in made:
                        one.wait_recv()

        start_gather("y")
        start_gather("z")
        send_layer("y", 0)
        gather("y", True)
        send_layer("z", 0)
        take_direct("y", 0)
        gather("z", True)
        for m in masks[1:]:
            take_direct("y", m)
        for s in ("y", "z"):
            finish_own(s)
        finish_halo("y")
        yield
        start_gather("u")
        send_layer("u", 0)
        for m in masks:
            take_direct("z", m)
        gather("u", True)
        for m in masks:
            take_relayed("z", m)
        finish_own("u")
        finish_halo("z")
        yield
        for m in masks:
            take_direct("u", m)
        for m in masks:
            take_relayed("u", m)
        finish_halo("u")
        yield
        for guard, made in remote:
            if guard is None:
                made.wait_send()
            else:
                pl.when(guard)(made.wait_send)
        yield

    plans = [schedule(me) for me in range(reps)]

    def advance():
        for me in range(reps):
            pl.when(rep == me)(functools.partial(next, plans[me]))

    down = lax.broadcasted_iota(jnp.int32, (tile, tile), 0)
    right = lax.broadcasted_iota(jnp.int32, (tile, tile), 1)
    identity = jnp.where(down == right, 1.5, 0.0).astype(jnp.float32)

    def multiply(left, right, store):
        def step(i, _):
            total = product_row(i, left, right, layer, rep, layers, rows, slots, band)
            for w in range(slots):
                store(i, w, pattern[i, w] == 1, total[:, w * tile : (w + 1) * tile])
            return 0

        lax.fori_loop(0, rows, step, 0)

    def store_update(i, w, good, value):
        value = -0.5 * value + jnp.where(rep * slots + w == half, identity, 0.0)
        u_wide[rows + i, rep * slots + w] = jnp.where(good, value, 0.0).astype(jnp.bfloat16)

    def store_inverse(i, w, good, value):
        z_next[i, w] = jnp.where(good, value, 0.0).astype(jnp.bfloat16)

    def store_square(i, w, good, value):
        y_next[i, w] = jnp.where(good, value, 0.0).astype(jnp.bfloat16)

    advance()
    multiply(z_wide, y_wide, store_update)
    advance()
    multiply(u_wide, z_wide, store_inverse)
    advance()
    multiply(y_wide, u_wide, store_square)
    advance()
    assert len(keys) <= send_sems.shape[0]


def product_row(i, left, right, layer, rep, layers, rows, slots, band):
    half = band // 2
    step = 4
    total = None
    for first in range(0, band, step):
        wide = jnp.concatenate([left[rows + i, u] for u in range(first, first + step)], axis=1)
        tall = []
        for u in range(first, first + step):
            row = layer * rows + i - half + u
            inside = jnp.logical_and(row >= 0, row < layers * rows)
            tiles = []
            for w in range(slots):
                v = rep * slots + w + half - u
                good = jnp.logical_and(inside, jnp.logical_and(v >= 0, v < band))
                part = right[i + u + rows - half, lax.rem(v + band, band)]
                tiles.append(jnp.where(good, part, jnp.zeros_like(part)))
            tall.append(jnp.concatenate(tiles, axis=1))
        piece = jnp.dot(wide, jnp.concatenate(tall, axis=0), preferred_element_type=jnp.float32)
        total = piece if total is None else total + piece
    return total


PAIRED_SEMAPHORES = 208


def block_spans(rows, band):
    lower = {a: (0, band // 2 - a) for a in range(rows)}
    upper = {a: (band - a, band) for a in range(1, rows)}
    return lower, upper


def paired_kernel(
    layers, reps, refs_shape, pattern, z_own, y_own, z_next, y_next,
    y_wide, z_wide, u_wide, z_sum, y_sum, z_out, y_out, z_in, y_in, send_sems, recv_sems,
):
    rows, slots, tile = refs_shape
    band = slots * reps
    half = band // 2
    step = 2
    chunks = [(a, a + step) for a in range(0, rows, step)]
    layer, rep = lax.axis_index("layer"), lax.axis_index("rep")
    after, before = lax.rem(layer + 1, layers), lax.rem(layer + layers - 1, layers)
    may_send = {1: layer + 1 < layers, -1: layer > 0}
    may_take = {1: layer > 0, -1: layer + 1 < layers}
    wides = {"y": y_wide, "z": z_wide, "u": u_wide}
    lower, upper = block_spans(rows, band)
    keys = {}

    barrier = pltpu.get_barrier_semaphore()
    for place in (after, before):
        pl.semaphore_signal(barrier, inc=1, device_id={"layer": place}, device_id_type=MESH)
    for flip in (1, 2):
        partner = rep + flip * (1 - 2 * lax.rem(lax.div(rep, flip), 2))
        pl.semaphore_signal(barrier, inc=1, device_id={"rep": partner}, device_id_type=MESH)

    def keep(own, wide):
        def row(i, _):
            for w in range(slots):
                part = own[i, w]
                wide[rows + i, rep * slots + w] = jnp.where(pattern[i, w] == 1, part, jnp.zeros_like(part))
            return 0

        lax.fori_loop(0, rows, row, 0)

    def schedule(me):
        chip = me // 2
        remote = []

        def base(side):
            return 0 if side == 1 else 2 * rows

        def own_side(who):
            return -1 if who // 2 == 0 else 1

        def own_spans(who):
            return lower if who // 2 == 0 else upper

        def cut(spans, q, chunk):
            kept = {a: spans[a] for a in spans if chunk[0] <= a < chunk[1]}
            return rectangles(kept, q * slots, (q + 1) * slots)

        def needs(who, side):
            low = who // 2 * 2 * slots
            return reached(rows, band, low, low + 2 * slots)[side]

        def sent(s, who, side, n):
            if s == "y":
                return needs(who, side)
            return own_spans(who) if n == 0 and side == own_side(who) else {}

        def extra(who):
            if who // 2:
                return {}
            need = needs(who, -1)
            return {a: (need[a][1] if a in need else 0, lower[a][1]) for a in lower}

        def relayed(who):
            side = own_side(who)
            need, have = needs(who ^ 2, side), own_spans(who)
            found = {}
            for a in have:
                if a in need:
                    lo, hi = max(need[a][0], have[a][0]), min(need[a][1], have[a][1])
                    if lo < hi:
                        found[a] = (lo, hi)
            return found

        def copy(key, src, dst, device):
            n = keys.setdefault(key, len(keys))
            return lambda: pltpu.make_async_remote_copy(
                src_ref=src, dst_ref=dst, send_sem=send_sems.at[0], recv_sem=recv_sems.at[n],
                device_id=device, device_id_type=MESH,
            )

        def begin(guard, made):
            if not made:
                return
            remote.append((guard, made))

            def go():
                for one in made:
                    one().start()

            go() if guard is None else pl.when(guard)(go)

        def take(guard, made, onward=()):
            if not made:
                return
            remote.append((guard, list(onward)))

            def go():
                for one in made:
                    one().wait_recv()
                for one in onward:
                    one().start()

            go() if guard is None else pl.when(guard)(go)

        def shard(s, q, chunk):
            return wides[s].at[pl.ds(rows + chunk[0], chunk[1] - chunk[0]), pl.ds(q * slots, slots)]

        def swap(s, q, chunk):
            part = shard(s, q, chunk)
            return copy(("swap", s, chunk), part, part, {"rep": me ^ 2})

        def pair(s, q, chunk):
            part = shard(s, q, chunk)
            return copy(("pair", s, chunk), part, part, {"rep": me ^ 1})

        def pass_pair(s, q, chunk):
            part = shard(s, q, chunk)
            return copy(("pass", s, chunk), part, part, {"rep": me ^ 1})

        def boxes(name, s, side, n, chunk, pieces, device, start):
            made = []
            for k, (a, b, lo, hi) in enumerate(pieces):
                src = wides[s].at[pl.ds(start + a, b - a), pl.ds(lo, hi - lo)]
                dst = wides[s].at[pl.ds(base(side) + a, b - a), pl.ds(lo, hi - lo)]
                made.append(copy((name, s, side, n, chunk, k), src, dst, device))
            return made

        def group(who, n):
            return who ^ 2 if n else who

        def to_layer(s, side, n, chunk):
            pieces = cut(sent(s, me, side, n), group(me, n), chunk)
            return boxes("x", s, side, n, chunk, pieces, {"layer": after if side == 1 else before}, rows)

        def layer_pass(s, side, n, chunk, who):
            pieces = cut(sent(s, who, side, n), group(who, n), chunk)
            return boxes("xp", s, side, n, chunk, pieces, {"rep": me ^ 1}, base(side))

        def extra_to_layer():
            return boxes("e", "y", -1, 0, 0, cut(extra(me), me, (0, rows)), {"layer": before}, rows)

        def extra_pass(who):
            return boxes("ep", "y", -1, 0, 0, cut(extra(who), who, (0, rows)), {"rep": me ^ 1}, 2 * rows)

        def relay(s, chunk, who):
            pieces = cut(relayed(who), who, chunk)
            side = own_side(who)
            return boxes("r", s, side, 0, chunk, pieces, {"rep": me ^ 2}, base(side))

        def relay_pass(s, chunk, who):
            pieces = cut(relayed(who), who, chunk)
            side = own_side(who)
            return boxes("rp", s, side, 0, chunk, pieces, {"rep": me ^ 1}, base(side))

        def partial_out(s, chunk):
            source, target = (z_out, z_in) if s == "z" else (y_out, y_in)
            made = []
            for k, (a, b, lo, hi) in enumerate(cut(own_spans(me), me, chunk)):
                at = (pl.ds(a, b - a), pl.ds(lo - me * slots, hi - lo))
                place = after if chip == 0 else before
                made.append(copy(("p", s, chunk, k), source.at[at], target.at[at], {"layer": place}))
            return made

        def start_swap(s, chunk):
            begin(None, [swap(s, me, chunk)])

        def start_pair(s, chunk):
            begin(None, [pair(s, me, chunk)])

        def end_swap(s, chunk):
            take(None, [swap(s, me ^ 2, chunk)], [pass_pair(s, me ^ 2, chunk)])

        def send_layer(s, n, chunk):
            for side in (1, -1):
                begin(may_send[side], to_layer(s, side, n, chunk))

        def take_layer(s, n, chunk):
            for side in (1, -1):
                onward = layer_pass(s, side, n, chunk, me)
                if s != "y":
                    onward = onward + relay(s, chunk, me)
                take(may_take[side], to_layer(s, side, n, chunk), onward)

        def take_layer_pass(s, n, chunk):
            for side in (1, -1):
                take(may_take[side], layer_pass(s, side, n, chunk, me ^ 1))

        def take_relay(s, chunk):
            take(may_take[own_side(me ^ 2)], relay(s, chunk, me ^ 2), relay_pass(s, chunk, me ^ 2))

        def take_relay_pass(s, chunk):
            take(may_take[own_side(me ^ 2)], relay_pass(s, chunk, me ^ 3))

        out_side = 1 if chip == 0 else -1

        for chunk in chunks:
            start_swap("y", chunk)
            send_layer("y", 0, chunk)
        for chunk in chunks:
            start_pair("y", chunk)
        yield
        for chunk in chunks:
            start_swap("z", chunk)
        for chunk in chunks:
            start_pair("z", chunk)
        for chunk in chunks:
            end_swap("y", chunk)
            send_layer("y", 1, chunk)
        for n, chunk in enumerate(chunks):
            take_layer("y", 0, chunk)
        for n, chunk in enumerate(chunks):
            end_swap("z", chunk)
            take_layer("y", 1, chunk)
        for chunk in chunks:
            take(None, [pair("y", me ^ 1, chunk)])
            take(None, [pass_pair("y", me ^ 3, chunk)])
            take(None, [pair("z", me ^ 1, chunk)])
            for n in (0, 1):
                take_layer_pass("y", n, chunk)
        begin(may_send[-1], extra_to_layer())
        for chunk in chunks:
            send_layer("z", 0, chunk)
        for chunk in chunks:
            take(None, [pass_pair("z", me ^ 3, chunk)])
            yield
            start_swap("u", chunk)
            start_pair("u", chunk)
            send_layer("u", 0, chunk)
        take(may_take[-1], extra_to_layer(), extra_pass(me))
        for n, chunk in enumerate(chunks):
            take_layer("z", 0, chunk)
            end_swap("u", chunk)
            take(None, [pair("u", me ^ 1, chunk)])
            take(None, [pass_pair("u", me ^ 3, chunk)])
            yield
        take(may_take[-1], extra_pass(me ^ 1))
        for chunk in chunks[: len(chunks) // 2]:
            take_layer("u", 0, chunk)
        for chunk in chunks[: len(chunks) // 2]:
            take_layer_pass("u", 0, chunk)
        yield
        for chunk in chunks[: len(chunks) // 2]:
            begin(may_send[out_side], partial_out("z", chunk))
        for chunk in chunks[len(chunks) // 2 :]:
            take_layer("u", 0, chunk)
        for chunk in chunks[len(chunks) // 2 :]:
            take_layer_pass("u", 0, chunk)
        yield
        for chunk in chunks[len(chunks) // 2 :]:
            begin(may_send[out_side], partial_out("z", chunk))
        yield
        for chunk in chunks:
            begin(may_send[out_side], partial_out("y", chunk))
        for chunk in chunks:
            take_relay("z", chunk)
        yield
        for chunk in chunks:
            take_layer_pass("z", 0, chunk)
            take_relay("u", chunk)
        for chunk in chunks:
            take_relay_pass("z", chunk)
            take_relay_pass("u", chunk)
        yield
        for chunk in chunks:
            take(may_take[out_side], partial_out("z", chunk))
        yield
        for chunk in chunks:
            take(may_take[out_side], partial_out("y", chunk))
        yield
        for guard, made in remote:

            def end(made=made):
                for one in made:
                    one().wait_send()

            if made:
                end() if guard is None else pl.when(guard)(end)
        yield

    plans = [schedule(me) for me in range(reps)]

    def advance():
        for me in range(reps):
            pl.when(rep == me)(functools.partial(next, plans[me]))

    down = lax.broadcasted_iota(jnp.int32, (tile, tile), 0)
    right_at = lax.broadcasted_iota(jnp.int32, (tile, tile), 1)
    identity = jnp.where(down == right_at, 1.5, 0.0).astype(jnp.float32)
    zero = jnp.zeros((tile, tile), jnp.bfloat16)

    def multiply(lefts, rights):
        wide = jnp.concatenate(lefts, axis=1)
        tall = jnp.concatenate([jnp.concatenate(one, axis=1) for one in rights], axis=0)
        return jnp.dot(wide, tall, preferred_element_type=jnp.float32)

    def own_part(i, left, right):
        lefts, rights = [], []
        for t in range(rows):
            u = half - i + t
            lefts.append(left[rows + i, u])
            line = []
            for w in range(slots):
                v = rep * slots + w + i - t
                good = jnp.logical_and(v >= 0, v < band)
                line.append(jnp.where(good, right[rows + t, lax.rem(v + band, band)], zero))
            rights.append(line)
        return multiply(lefts, rights)

    def halo_part(i, left, right, inner):
        lefts, rights = [], []
        for t in range(rows):
            u = lax.rem(t - i + band, band)
            lefts.append(left[rows + i, u])
            line = []
            row = layer * rows + i - half + u
            inside = jnp.logical_and(row >= 0, row < layers * rows)
            for w in range(slots):
                v = rep * slots + w + half - u
                good = jnp.logical_and(inside, jnp.logical_and(v >= 0, v < band))
                if inner:
                    k = i - half + rep * slots + w
                    good = jnp.logical_and(good, jnp.logical_and(k >= 0, k < rows))
                line.append(jnp.where(good, right[i + u, lax.rem(v + band, band)], zero))
            rights.append(line)
        return multiply(lefts, rights)

    def split(total, w):
        return total[:, w * tile : (w + 1) * tile]

    def update_rows(chunk):
        def row(i, _):
            total = own_part(i, z_wide, y_wide) + halo_part(i, z_wide, y_wide, False)
            for w in range(slots):
                value = -0.5 * split(total, w) + jnp.where(rep * slots + w == half, identity, 0.0)
                value = jnp.where(pattern[i, w] == 1, value, 0.0)
                u_wide[rows + i, rep * slots + w] = value.astype(jnp.bfloat16)
            return 0

        lax.fori_loop(chunk[0], chunk[1], row, 0)

    def own_rows(left, right, total, chunk):
        def row(i, _):
            value = own_part(i, left, right)
            for w in range(slots):
                total[i, w] = split(value, w)
            return 0

        lax.fori_loop(chunk[0], chunk[1], row, 0)

    def halo_rows(left, right, total):
        def row(i, _):
            value = halo_part(i, left, right, True)
            for w in range(slots):
                total[i, w] += split(value, w)
            return 0

        lax.fori_loop(0, rows, row, 0)

    def partial_rows(left, right, out, chunk):
        chip = lax.div(rep, 2)

        def row(i, _):
            lefts, rights = [], []
            for t in range(rows):
                u = t + half * chip
                part = left[2 * rows * (1 - chip) + i, u]
                lefts.append(jnp.where(lax.div(i + t, rows) == chip, part, zero))
                j = lax.rem(i + t, rows)
                rights.append([
                    right[rows + j, rep * slots + w + half - u] for w in range(slots)
                ])
            value = multiply(lefts, rights)
            for w in range(slots):
                out[i, w] = split(value, w).astype(jnp.bfloat16)
            return 0

        lax.fori_loop(chunk[0], chunk[1], row, 0)

    def finish(total, part, result):
        def row(i, _):
            for w in range(slots):
                k = i - half + rep * slots + w
                below = jnp.logical_and(k < 0, layer > 0)
                above = jnp.logical_and(k >= rows, layer + 1 < layers)
                more = jnp.where(jnp.logical_or(below, above), part[i, w].astype(jnp.float32), 0.0)
                value = jnp.where(pattern[i, w] == 1, total[i, w] + more, 0.0)
                result[i, w] = value.astype(jnp.bfloat16)
            return 0

        lax.fori_loop(0, rows, row, 0)

    keep(y_own, y_wide)
    pl.semaphore_wait(barrier, 4)
    advance()
    keep(z_own, z_wide)
    for chunk in chunks:
        advance()
        update_rows(chunk)
    for chunk in chunks:
        advance()
        own_rows(u_wide, z_wide, z_sum, chunk)
    advance()
    middle = rows // 2
    partial_rows(u_wide, z_wide, z_out, (0, middle))
    advance()
    partial_rows(u_wide, z_wide, z_out, (middle, rows))
    advance()
    partial_rows(y_wide, u_wide, y_out, (0, rows))
    advance()
    own_rows(y_wide, u_wide, y_sum, (0, rows))
    advance()
    halo_rows(u_wide, z_wide, z_sum)
    halo_rows(y_wide, u_wide, y_sum)
    advance()
    finish(z_sum, z_in, z_next)
    advance()
    finish(y_sum, y_in, y_next)
    advance()
    assert len(keys) <= recv_sems.shape[0]


def solution(mesh):
    layers, reps = mesh.shape["layer"], mesh.shape["rep"]

    def body(inverse_root, square_root, pattern):
        rows, slots = pattern.shape
        tile = inverse_root.shape[2:]
        local = jax.ShapeDtypeStruct((rows, slots) + tile, jnp.bfloat16)
        wide = pltpu.VMEM((3 * rows, slots * reps) + tile, jnp.bfloat16)
        sems = [pltpu.SemaphoreType.DMA((SEMAPHORES,))] * 2
        paired = reps == 4 and 2 * rows == slots * reps and rows % 4 == 0
        kernel, extra = step_kernel, []
        if paired:
            kernel = paired_kernel
            extra = [pltpu.VMEM((rows, slots) + tile, jnp.float32)] * 2
            extra += [pltpu.VMEM((rows, slots) + tile, jnp.bfloat16)] * 4
            sems = [pltpu.SemaphoreType.DMA((1,)), pltpu.SemaphoreType.DMA((PAIRED_SEMAPHORES,))]
        return pl.pallas_call(
            functools.partial(kernel, layers, reps, (rows, slots, tile[0])),
            out_shape=(local, local),
            in_specs=[SMEM, VMEM, VMEM],
            out_specs=(VMEM, VMEM),
            scratch_shapes=[wide, wide, wide] + extra + sems,
            compiler_params=pltpu.CompilerParams(
                collective_id=0, has_side_effects=True, vmem_limit_bytes=60 * 1024 * 1024
            ),
            name="newton_step",
        )(pattern, inverse_root, square_root)

    placed = P("layer", "rep", None, None)
    return jax.shard_map(
        body,
        mesh=mesh,
        in_specs=(placed, placed, P("layer", "rep")),
        out_specs=(placed, placed),
        check_vma=False,
    )
```

```python
import functools

import jax
import jax.numpy as jnp
from jax import lax
from jax.experimental import pallas as pl
from jax.experimental.pallas import tpu as pltpu
from jax.sharding import PartitionSpec as P

MESH = pl.DeviceIdType.MESH
VMEM = pl.BlockSpec(memory_space=pltpu.VMEM)
SMEM = pl.BlockSpec(memory_space=pltpu.SMEM)
SEMAPHORES = 256


def reached(rows, band, low, high):
    half = band // 2
    found = {1: {}, -1: {}}
    for i in range(rows):
        for u in range(band):
            j = i - half + u
            if 0 <= j < rows:
                continue
            assert -rows <= j < 2 * rows
            side, a = (1, j + rows) if j < 0 else (-1, j - rows)
            for w in range(low, high):
                v = w + half - u
                if 0 <= v < band:
                    lo, hi = found[side].get(a, (v, v + 1))
                    found[side][a] = (min(lo, v), max(hi, v + 1))
    return found


def rectangles(spans, first, last):
    cut = []
    for a in sorted(spans):
        lo, hi = max(spans[a][0], first), min(spans[a][1], last)
        if lo >= hi:
            continue
        if cut and cut[-1][1] == a and cut[-1][2:] == (lo, hi):
            cut[-1] = (cut[-1][0], a + 1, lo, hi)
        else:
            cut.append((a, a + 1, lo, hi))
    return cut


class Later:
    def __init__(self, make, args=None):
        self.make, self.args = make, args

    def __call__(self, *args):
        return Later(self.make, args)

    def start(self):
        self.make(*self.args).start()

    def wait_recv(self):
        self.make(*self.args).wait_recv()

    def wait_send(self):
        self.make(*self.args).wait_send()


def step_kernel(layers, reps, refs_shape, pattern, z_own, y_own, z_next, y_next, y_wide, z_wide, u_wide, send_sems, recv_sems):
    rows, slots, tile = refs_shape
    band = slots * reps
    half = band // 2
    layer, rep = lax.axis_index("layer"), lax.axis_index("rep")
    after, before = lax.rem(layer + 1, layers), lax.rem(layer + layers - 1, layers)
    may_send = {1: layer + 1 < layers, -1: layer > 0}
    may_take = {1: layer > 0, -1: layer + 1 < layers}
    bits = []
    bit = reps // 2
    while bit >= 2:
        bits.append(bit)
        bit //= 2
    masks = list(range(0, reps, 2))
    keys = {}
    wides = {"y": y_wide, "z": z_wide, "u": u_wide}
    relayed = ("z", "u") if reps == 4 else ()

    def keep(i, _):
        for w in range(slots):
            good = pattern[i, w] == 1
            for own, wide in ((y_own, y_wide), (z_own, z_wide)):
                part = own[i, w]
                wide[rows + i, rep * slots + w] = jnp.where(good, part, jnp.zeros_like(part))
        return 0

    lax.fori_loop(0, rows, keep, 0)

    barrier = pltpu.get_barrier_semaphore()
    for place in (after, before):
        pl.semaphore_signal(barrier, inc=1, device_id={"layer": place}, device_id_type=MESH)
    for flip in [1] + bits:
        partner = rep + flip * (1 - 2 * lax.rem(lax.div(rep, flip), 2))
        pl.semaphore_signal(barrier, inc=1, device_id={"rep": partner}, device_id_type=MESH)
    pl.semaphore_wait(barrier, 3 + len(bits))

    def schedule(me):
        chip = me // 2
        remote = []
        need = reached(rows, band, chip * 2 * slots, (chip + 1) * 2 * slots)
        union = reached(rows, band, 0, band)
        other = reached(rows, band, (1 - chip) * 2 * slots, (2 - chip) * 2 * slots) if relayed else None
        direct_side = 1 if chip == 0 else -1

        def spans(s, side):
            if s not in relayed:
                return need[side]
            return union[side] if side == direct_side else {}

        def arriving(s, side):
            return spans(s, side) or need[side]

        def cut(which, q):
            return rectangles(which, q * slots, (q + 1) * slots)

        def base(side):
            return 0 if side == 1 else 2 * rows

        def copy(key, src, dst, device):
            n = keys.setdefault(key, len(keys))
            return pltpu.make_async_remote_copy(
                src_ref=src, dst_ref=dst, send_sem=send_sems.at[n], recv_sem=recv_sems.at[n],
                device_id=device, device_id_type=MESH,
            )

        def begin(guard, made):
            remote.append((guard, made))
            if guard is None:
                made.start()
            else:
                pl.when(guard)(made.start)

        def shard(s, q):
            return wides[s].at[pl.ds(rows, rows), pl.ds(q * slots, slots)]

        @Later
        def across(s, m, bit):
            part = shard(s, me ^ bit ^ m)
            return copy(("y", s, m), part, part, {"rep": me ^ bit})

        @Later
        def across_in(s, m, bit):
            part = shard(s, me ^ m)
            return copy(("y", s, m), part, part, {"rep": me ^ bit})

        @Later
        def to_core(s, m):
            part = shard(s, me ^ m)
            return copy(("d", s, m), part, part, {"rep": me ^ 1})

        @Later
        def to_core_in(s, m):
            part = shard(s, me ^ 1 ^ m)
            return copy(("d", s, m), part, part, {"rep": me ^ 1})

        @Later
        def to_layer(s, side, m, k, piece):
            a, b, lo, hi = piece
            src = wides[s].at[pl.ds(rows + a, b - a), pl.ds(lo, hi - lo)]
            dst = wides[s].at[pl.ds(base(side) + a, b - a), pl.ds(lo, hi - lo)]
            return copy(("x", s, side, m, k), src, dst, {"layer": after if side == 1 else before})

        @Later
        def relay(s, side, m, k, piece):
            a, b, lo, hi = piece
            part = wides[s].at[pl.ds(base(side) + a, b - a), pl.ds(lo, hi - lo)]
            return copy(("r", s, side, m, k), part, part, {"rep": me ^ 2})

        @Later
        def halo_to_core(s, side, m, q):
            pieces = cut(arriving(s, side), q)
            a, b = min(c[0] for c in pieces), max(c[1] for c in pieces)
            part = wides[s].at[pl.ds(base(side) + a, b - a), pl.ds(q * slots, slots)]
            return copy(("h", s, side, m), part, part, {"rep": me ^ 1})

        def send_layer(s, m):
            for side in (1, -1):
                for k, piece in enumerate(cut(spans(s, side), me ^ m)):
                    begin(may_send[side], to_layer(s, side, m, k, piece))

        def take_direct(s, m):
            for side in (1, -1):
                pieces = cut(spans(s, side), me ^ m)
                if pieces:
                    made = [to_layer(s, side, m, k, piece) for k, piece in enumerate(pieces)]
                    onward = [halo_to_core(s, side, m, me ^ m)]
                    if s in relayed:
                        onward += [
                            relay(s, side, m ^ 2, k, piece)
                            for k, piece in enumerate(cut(other[side], me ^ m))
                        ]
                    pass_on(side, made, onward)

        def take_relayed(s, m):
            for side in (1, -1):
                if s in relayed and side != direct_side:
                    pieces = cut(need[side], me ^ m)
                    if pieces:
                        made = [relay(s, side, m, k, piece) for k, piece in enumerate(pieces)]
                        pass_on(side, made, [halo_to_core(s, side, m, me ^ m)])

        def pass_on(side, made, onward):
            remote.extend((may_take[side], o) for o in onward)

            @pl.when(may_take[side])
            def _():
                for one in made:
                    one.wait_recv()
                for one in onward:
                    one.start()

        def start_gather(s):
            if bits:
                begin(None, across(s, bits[0], bits[0]))
            begin(None, to_core(s, 0))

        def gather(s, halo):
            held = [0]
            for n, bit in enumerate(bits):
                if n > 0:
                    for m in held:
                        begin(None, across(s, m ^ bit, bit))
                fresh = [m ^ bit for m in held]
                for m in fresh:
                    across_in(s, m, bit).wait_recv()
                    begin(None, to_core(s, m))
                    if halo:
                        send_layer(s, m)
                held = held + fresh

        def finish_own(s):
            for m in masks:
                to_core_in(s, m).wait_recv()

        def finish_halo(s):
            for side in (1, -1):
                made = [
                    halo_to_core(s, side, m, me ^ 1 ^ m)
                    for m in masks
                    if cut(arriving(s, side), me ^ 1 ^ m)
                ]

                @pl.when(may_take[side])
                def _():
                    for one in made:
                        one.wait_recv()

        start_gather("y")
        start_gather("z")
        send_layer("y", 0)
        gather("y", True)
        send_layer("z", 0)
        take_direct("y", 0)
        gather("z", True)
        for m in masks[1:]:
            take_direct("y", m)
        for s in ("y", "z"):
            finish_own(s)
        finish_halo("y")
        yield
        start_gather("u")
        send_layer("u", 0)
        for m in masks:
            take_direct("z", m)
        gather("u", True)
        for m in masks:
            take_relayed("z", m)
        finish_own("u")
        finish_halo("z")
        yield
        for m in masks:
            take_direct("u", m)
        for m in masks:
            take_relayed("u", m)
        finish_halo("u")
        yield
        for guard, made in remote:
            if guard is None:
                made.wait_send()
            else:
                pl.when(guard)(made.wait_send)
        yield

    plans = [schedule(me) for me in range(reps)]

    def advance():
        for me in range(reps):
            pl.when(rep == me)(functools.partial(next, plans[me]))

    down = lax.broadcasted_iota(jnp.int32, (tile, tile), 0)
    right = lax.broadcasted_iota(jnp.int32, (tile, tile), 1)
    identity = jnp.where(down == right, 1.5, 0.0).astype(jnp.float32)

    def multiply(left, right, store):
        def step(i, _):
            total = product_row(i, left, right, layer, rep, layers, rows, slots, band)
            for w in range(slots):
                store(i, w, pattern[i, w] == 1, total[:, w * tile : (w + 1) * tile])
            return 0

        lax.fori_loop(0, rows, step, 0)

    def store_update(i, w, good, value):
        value = -0.5 * value + jnp.where(rep * slots + w == half, identity, 0.0)
        u_wide[rows + i, rep * slots + w] = jnp.where(good, value, 0.0).astype(jnp.bfloat16)

    def store_inverse(i, w, good, value):
        z_next[i, w] = jnp.where(good, value, 0.0).astype(jnp.bfloat16)

    def store_square(i, w, good, value):
        y_next[i, w] = jnp.where(good, value, 0.0).astype(jnp.bfloat16)

    advance()
    multiply(z_wide, y_wide, store_update)
    advance()
    multiply(u_wide, z_wide, store_inverse)
    advance()
    multiply(y_wide, u_wide, store_square)
    advance()
    assert len(keys) <= send_sems.shape[0]


def product_row(i, left, right, layer, rep, layers, rows, slots, band):
    half = band // 2
    step = 4
    total = None
    for first in range(0, band, step):
        wide = jnp.concatenate([left[rows + i, u] for u in range(first, first + step)], axis=1)
        tall = []
        for u in range(first, first + step):
            row = layer * rows + i - half + u
            inside = jnp.logical_and(row >= 0, row < layers * rows)
            tiles = []
            for w in range(slots):
                v = rep * slots + w + half - u
                good = jnp.logical_and(inside, jnp.logical_and(v >= 0, v < band))
                part = right[i + u + rows - half, lax.rem(v + band, band)]
                tiles.append(jnp.where(good, part, jnp.zeros_like(part)))
            tall.append(jnp.concatenate(tiles, axis=1))
        piece = jnp.dot(wide, jnp.concatenate(tall, axis=0), preferred_element_type=jnp.float32)
        total = piece if total is None else total + piece
    return total


PAIRED_SEMAPHORES = 144
VMEM_BYTES = 52 * 1024 * 1024


def block_spans(rows, band):
    lower = {a: (0, band // 2 - a) for a in range(rows)}
    upper = {a: (band - a, band) for a in range(1, rows)}
    return lower, upper


def paired_kernel(
    layers, reps, refs_shape, pattern, z_own, y_own, z_next, y_next,
    y_wide, z_wide, u_wide, z_sum, y_sum, c_out, z_out, y_out, c_in, z_in, y_in, send_sems, recv_sems,
):
    rows, slots, tile = refs_shape
    band = slots * reps
    half = band // 2
    step = 2
    chunks = [(a, a + step) for a in range(0, rows, step)]
    layer, rep = lax.axis_index("layer"), lax.axis_index("rep")
    after, before = lax.rem(layer + 1, layers), lax.rem(layer + layers - 1, layers)
    may_send = {1: layer + 1 < layers, -1: layer > 0}
    may_take = {1: layer > 0, -1: layer + 1 < layers}
    wides = {"y": y_wide, "z": z_wide, "u": u_wide}
    partials = {"c": (c_out, c_in), "z": (z_out, z_in), "y": (y_out, y_in)}
    lower, upper = block_spans(rows, band)
    keys = {}

    barrier = pltpu.get_barrier_semaphore()
    for place in (after, before):
        pl.semaphore_signal(barrier, inc=1, device_id={"layer": place}, device_id_type=MESH)
    for flip in (1, 2):
        partner = rep + flip * (1 - 2 * lax.rem(lax.div(rep, flip), 2))
        pl.semaphore_signal(barrier, inc=1, device_id={"rep": partner}, device_id_type=MESH)

    def keep(own, wide):
        def row(i, _):
            for w in range(slots):
                part = own[i, w]
                wide[rows + i, rep * slots + w] = jnp.where(pattern[i, w] == 1, part, jnp.zeros_like(part))
            return 0

        lax.fori_loop(0, rows, row, 0)

    class Parcel:
        def __init__(self, n, pairs, device):
            self.n, self.pairs, self.device = n, pairs, device

        def copies(self):
            for src, dst in self.pairs:
                yield pltpu.make_async_remote_copy(
                    src_ref=src, dst_ref=dst, send_sem=send_sems.at[0], recv_sem=recv_sems.at[self.n],
                    device_id=self.device, device_id_type=MESH,
                )

        def start(self):
            for one in self.copies():
                one.start()

        def wait_send(self):
            for one in self.copies():
                one.wait_send()

        def wait_recv(self):
            if len(self.pairs) == 1:
                next(self.copies()).wait_recv()
                return
            tiles = sum(dst.shape[0] * dst.shape[1] for _, dst in self.pairs)
            at = y_wide.at[pl.ds(0, 1), pl.ds(0, tiles)]
            Parcel(self.n, [(at, at)], self.device).wait_recv()

    def schedule(me):
        chip = me // 2
        remote = []

        def base(side):
            return 0 if side == 1 else 2 * rows

        def own_side(who):
            return -1 if who // 2 == 0 else 1

        def own_spans(who):
            return lower if who // 2 == 0 else upper

        def cut(spans, q, chunk):
            kept = {a: spans[a] for a in spans if chunk[0] <= a < chunk[1]}
            return rectangles(kept, q * slots, (q + 1) * slots)

        def needs(who, side):
            low = who // 2 * 2 * slots
            return reached(rows, band, low, low + 2 * slots)[side]

        def sent(s, who, side, n):
            if side == own_side(who):
                return {} if n else own_spans(who)
            return shared(who ^ 2) if n and s == "y" else {}

        def shared(who):
            side = own_side(who)
            need, have = needs(who ^ 2, side), own_spans(who)
            found = {}
            for a in have:
                if a in need:
                    lo, hi = max(need[a][0], have[a][0]), min(need[a][1], have[a][1])
                    if lo < hi:
                        found[a] = (lo, hi)
            return found

        def copy(key, src, dst, device):
            return Parcel(keys.setdefault(key, len(keys)), [(src, dst)], device)

        def begin(guard, made):
            if not made:
                return
            remote.append((guard, made))

            def go():
                for one in made:
                    one.start()

            go() if guard is None else pl.when(guard)(go)

        def take(guard, made, onward=()):
            if not made:
                return
            remote.append((guard, list(onward)))

            def go():
                for one in made:
                    one.wait_recv()
                for one in onward:
                    one.start()

            go() if guard is None else pl.when(guard)(go)

        def shard(s, q, chunk):
            return wides[s].at[pl.ds(rows + chunk[0], chunk[1] - chunk[0]), pl.ds(q * slots, slots)]

        def swap(s, q, chunk):
            part = shard(s, q, chunk)
            return copy(("swap", s, chunk), part, part, {"rep": me ^ 2})

        def pair(s, q, chunk):
            part = shard(s, q, chunk)
            return copy(("pair", s, chunk), part, part, {"rep": me ^ 1})

        def pass_pair(s, q, chunk):
            part = shard(s, q, chunk)
            return copy(("pass", s, chunk), part, part, {"rep": me ^ 1})

        def parcel(key, pairs, device):
            return [Parcel(keys.setdefault(key, len(keys)), pairs, device)] if pairs else []

        def boxes(name, s, side, n, chunk, pieces, device, start):
            pairs = []
            for a, b, lo, hi in pieces:
                src = wides[s].at[pl.ds(start + a, b - a), pl.ds(lo, hi - lo)]
                dst = wides[s].at[pl.ds(base(side) + a, b - a), pl.ds(lo, hi - lo)]
                pairs.append((src, dst))
            return parcel((name, s, side, n, chunk), pairs, device)

        def group(who, n):
            return who ^ 2 if n else who

        def to_layer(s, side, n, chunk):
            pieces = cut(sent(s, me, side, n), group(me, n), chunk)
            return boxes("x", s, side, n, chunk, pieces, {"layer": after if side == 1 else before}, rows)

        def layer_pass(s, side, n, chunk, who):
            pieces = cut(sent(s, who, side, n), group(who, n), chunk)
            return boxes("xp", s, side, n, chunk, pieces, {"rep": me ^ 1}, base(side))

        def relay(s, chunk, who):
            pieces = cut(shared(who), who, chunk)
            side = own_side(who)
            return boxes("r", s, side, 0, chunk, pieces, {"rep": me ^ 2}, base(side))

        def relay_pass(s, chunk, who):
            pieces = cut(shared(who), who, chunk)
            side = own_side(who)
            return boxes("rp", s, side, 0, chunk, pieces, {"rep": me ^ 1}, base(side))

        def partial_out(s, chunk):
            source, target = partials[s]
            pairs = []
            for a, b, lo, hi in cut(own_spans(me), me, chunk):
                at = (pl.ds(a, b - a), pl.ds(lo - me * slots, hi - lo))
                pairs.append((source.at[at], target.at[at]))
            return parcel(("p", s, chunk), pairs, {"layer": after if chip == 0 else before})

        def start_swap(s, chunk):
            begin(None, [swap(s, me, chunk)])

        def start_pair(s, chunk):
            begin(None, [pair(s, me, chunk)])

        def end_swap(s, chunk):
            take(None, [swap(s, me ^ 2, chunk)], [pass_pair(s, me ^ 2, chunk)])

        def send_layer(s, n, chunk):
            for side in (1, -1):
                begin(may_send[side], to_layer(s, side, n, chunk))

        def take_layer(s, n, chunk):
            for side in (1, -1):
                take(may_take[side], to_layer(s, side, n, chunk), layer_pass(s, side, n, chunk, me))

        def take_layer_pass(s, n, chunk):
            for side in (1, -1):
                take(may_take[side], layer_pass(s, side, n, chunk, me ^ 1))

        def take_relay(s, chunk):
            take(may_take[own_side(me ^ 2)], relay(s, chunk, me ^ 2), relay_pass(s, chunk, me ^ 2))

        def take_relay_pass(s, chunk):
            take(may_take[own_side(me ^ 2)], relay_pass(s, chunk, me ^ 3))

        out_side = 1 if chip == 0 else -1

        for chunk in chunks:
            start_swap("y", chunk)
        yield
        for s in ("z", "y"):
            for chunk in chunks:
                send_layer(s, 0, chunk)
        for chunk in chunks:
            start_swap("z", chunk)
        for s in ("y", "z"):
            for chunk in chunks:
                start_pair(s, chunk)
        for chunk in chunks:
            end_swap("y", chunk)
            send_layer("y", 1, chunk)
        for chunk in chunks:
            take_layer("z", 0, chunk)
        for chunk in chunks:
            take(None, [pair("y", me ^ 1, chunk)])
            take(None, [pass_pair("y", me ^ 3, chunk)])
            take_layer_pass("z", 0, chunk)
        yield
        for chunk in chunks:
            begin(may_send[out_side], partial_out("c", chunk))
        for n, chunk in enumerate(chunks[:-1]):
            end_swap("z", chunk)
            take_layer("y", 1, chunk)
            take(None, [pair("z", me ^ 1, chunk)])
            if n:
                take(None, [pass_pair("z", me ^ 3, chunks[n - 1])])
                yield
        take_layer("y", 1, chunks[-1])
        for chunk in chunks:
            if chip == 1:
                take_layer("y", 0, chunk)
            take_layer_pass("y", 1, chunk)
        if chip == 1:
            for chunk in chunks:
                take_layer_pass("y", 0, chunk)
        take(None, [pair("z", me ^ 1, chunks[-1])])
        take(None, [pass_pair("z", me ^ 3, chunks[-2])])
        for chunk in chunks:
            if chunk == chunks[-1]:
                end_swap("z", chunk)
                take(None, [pass_pair("z", me ^ 3, chunk)])
            if chip == 0:
                take_layer("y", 0, chunk)
                take_layer_pass("y", 0, chunk)
            take(may_take[out_side], partial_out("c", chunk))
            yield
            start_swap("u", chunk)
            start_pair("u", chunk)
        for chunk in chunks:
            send_layer("u", 0, chunk)
        for chunk in chunks:
            begin(may_take[own_side(me)], relay("z", chunk, me))
        first, last = chunks[: len(chunks) // 2], chunks[len(chunks) // 2 :]
        for some in (first, last):
            for chunk in some:
                if chunk != chunks[-1]:
                    end_swap("u", chunk)
                take_layer("u", 0, chunk)
            for chunk in some:
                take_layer_pass("u", 0, chunk)
            yield
        for chunk in chunks:
            begin(may_send[out_side], partial_out("z", chunk))
        for chunk in chunks[:: 1 if chip == 0 else -1]:
            begin(may_take[own_side(me)], relay("u", chunk, me))
        for chunk in chunks:
            if chunk == chunks[-1]:
                end_swap("u", chunk)
            take(None, [pair("u", me ^ 1, chunk)])
            take(None, [pass_pair("u", me ^ 3, chunk)])
        yield
        for chunk in chunks:
            begin(may_send[out_side], partial_out("y", chunk))
        yield
        for chunk in chunks:
            take_relay("z", chunk)
        yield
        for chunk in chunks:
            take_relay_pass("z", chunk)
        yield
        arriving = chunks[:: 1 if chip == 1 else -1]
        for chunk in arriving[:-1]:
            take_relay("u", chunk)
        for n, chunk in enumerate(arriving):
            if n == len(arriving) - 2:
                take_relay("u", arriving[-1])
            take_relay_pass("u", chunk)
            yield
        for chunk in chunks:
            take(may_take[out_side], partial_out("z", chunk))
        yield
        for chunk in chunks:
            take(may_take[out_side], partial_out("y", chunk))
        yield
        for guard, made in remote:

            def end(made=made):
                for one in made:
                    one.wait_send()

            if made:
                end() if guard is None else pl.when(guard)(end)
        yield

    plans = [schedule(me) for me in range(reps)]

    def advance():
        for me in range(reps):
            pl.when(rep == me)(functools.partial(next, plans[me]))

    down = lax.broadcasted_iota(jnp.int32, (tile, tile), 0)
    right_at = lax.broadcasted_iota(jnp.int32, (tile, tile), 1)
    identity = jnp.where(down == right_at, 1.5, 0.0).astype(jnp.float32)
    zero = jnp.zeros((tile, tile), jnp.bfloat16)

    def multiply(lefts, rights):
        wide = jnp.concatenate(lefts, axis=1)
        tall = jnp.concatenate([jnp.concatenate(one, axis=1) for one in rights], axis=0)
        return jnp.dot(wide, tall, preferred_element_type=jnp.float32)

    def own_part(i, left, right):
        lefts, rights = [], []
        for t in range(rows):
            u = half - i + t
            lefts.append(left[rows + i, u])
            line = []
            for w in range(slots):
                v = rep * slots + w + i - t
                good = jnp.logical_and(v >= 0, v < band)
                line.append(jnp.where(good, right[rows + t, lax.rem(v + band, band)], zero))
            rights.append(line)
        return multiply(lefts, rights)

    def halo_part(i, left, right):
        lefts, rights = [], []
        for t in range(rows):
            u = lax.rem(t - i + band, band)
            lefts.append(left[rows + i, u])
            line = []
            row = layer * rows + i - half + u
            inside = jnp.logical_and(row >= 0, row < layers * rows)
            for w in range(slots):
                v = rep * slots + w + half - u
                good = jnp.logical_and(inside, jnp.logical_and(v >= 0, v < band))
                k = i - half + rep * slots + w
                good = jnp.logical_and(good, jnp.logical_and(k >= 0, k < rows))
                line.append(jnp.where(good, right[i + u, lax.rem(v + band, band)], zero))
            rights.append(line)
        return multiply(lefts, rights)

    def split(total, w):
        return total[:, w * tile : (w + 1) * tile]

    def returned(part, i, w):
        k = i - half + rep * slots + w
        below = jnp.logical_and(k < 0, layer > 0)
        above = jnp.logical_and(k >= rows, layer + 1 < layers)
        return jnp.where(jnp.logical_or(below, above), part[i, w].astype(jnp.float32), 0.0)

    def update_rows(chunk):
        def row(i, _):
            total = halo_part(i, z_wide, y_wide)
            for w in range(slots):
                value = -0.5 * (split(total, w) + z_sum[i, w] + returned(c_in, i, w))
                value += jnp.where(rep * slots + w == half, identity, 0.0)
                value = jnp.where(pattern[i, w] == 1, value, 0.0)
                u_wide[rows + i, rep * slots + w] = value.astype(jnp.bfloat16)
            return 0

        lax.fori_loop(chunk[0], chunk[1], row, 0)

    def own_rows(left, right, total, chunk):
        def row(i, _):
            value = own_part(i, left, right)
            for w in range(slots):
                total[i, w] = split(value, w)
            return 0

        lax.fori_loop(chunk[0], chunk[1], row, 0)

    def halo_rows(left, right, total, n, turn):
        def row(r, _):
            i = n * step + r
            if turn:
                i = lax.div(rep, 2) * (2 * n * step + step - rows) + rows - step - n * step + r
            value = halo_part(i, left, right)
            for w in range(slots):
                total[i, w] += split(value, w)
            return 0

        lax.fori_loop(0, step if turn else rows, row, 0)

    def partial_rows(left, right, out, chunk):
        chip = lax.div(rep, 2)

        def row(i, _):
            lefts, rights = [], []
            for t in range(rows):
                u = t + half * chip
                part = left[2 * rows * (1 - chip) + i, u]
                lefts.append(jnp.where(lax.div(i + t, rows) == chip, part, zero))
                j = lax.rem(i + t, rows)
                rights.append([
                    right[rows + j, rep * slots + w + half - u] for w in range(slots)
                ])
            value = multiply(lefts, rights)
            for w in range(slots):
                out[i, w] = split(value, w).astype(jnp.bfloat16)
            return 0

        lax.fori_loop(chunk[0], chunk[1], row, 0)

    def finish(total, part, result):
        def row(i, _):
            for w in range(slots):
                value = jnp.where(pattern[i, w] == 1, total[i, w] + returned(part, i, w), 0.0)
                result[i, w] = value.astype(jnp.bfloat16)
            return 0

        lax.fori_loop(0, rows, row, 0)

    keep(y_own, y_wide)
    pl.semaphore_wait(barrier, 4)
    advance()
    keep(z_own, z_wide)
    middle = rows // 2
    advance()
    partial_rows(z_wide, y_wide, c_out, (0, rows))
    for chunk in chunks[:-2]:
        advance()
        own_rows(z_wide, y_wide, z_sum, chunk)
    for chunk in chunks:
        advance()
        if chunk == chunks[0]:
            own_rows(z_wide, y_wide, z_sum, chunks[-2])
        if chunk == chunks[-1]:
            own_rows(z_wide, y_wide, z_sum, chunk)
        update_rows(chunk)
    for chunk in ((0, middle), (middle, rows)):
        advance()
        partial_rows(u_wide, z_wide, z_out, chunk)
    advance()
    partial_rows(y_wide, u_wide, y_out, (0, rows))
    advance()
    own_rows(u_wide, z_wide, z_sum, (0, rows))
    advance()
    own_rows(y_wide, u_wide, y_sum, (0, rows))
    advance()
    halo_rows(u_wide, z_wide, z_sum, 0, False)
    for n in range(len(chunks)):
        advance()
        halo_rows(y_wide, u_wide, y_sum, n, True)
    advance()
    finish(z_sum, z_in, z_next)
    advance()
    finish(y_sum, y_in, y_next)
    advance()
    assert len(keys) <= recv_sems.shape[0]


def solution(mesh):
    layers, reps = mesh.shape["layer"], mesh.shape["rep"]

    def body(inverse_root, square_root, pattern):
        rows, slots = pattern.shape
        tile = inverse_root.shape[2:]
        local = jax.ShapeDtypeStruct((rows, slots) + tile, jnp.bfloat16)
        wide = pltpu.VMEM((3 * rows, slots * reps) + tile, jnp.bfloat16)
        sems = [pltpu.SemaphoreType.DMA((SEMAPHORES,))] * 2
        paired = reps == 4 and 2 * rows == slots * reps and rows % 4 == 0
        kernel, extra = step_kernel, []
        if paired:
            kernel = paired_kernel
            extra = [pltpu.VMEM((rows, slots) + tile, jnp.float32)] * 2
            extra += [pltpu.VMEM((rows, slots) + tile, jnp.bfloat16)] * 6
            sems = [pltpu.SemaphoreType.DMA((1,)), pltpu.SemaphoreType.DMA((PAIRED_SEMAPHORES,))]
        return pl.pallas_call(
            functools.partial(kernel, layers, reps, (rows, slots, tile[0])),
            out_shape=(local, local),
            in_specs=[SMEM, VMEM, VMEM],
            out_specs=(VMEM, VMEM),
            scratch_shapes=[wide, wide, wide] + extra + sems,
            compiler_params=pltpu.CompilerParams(
                collective_id=0, has_side_effects=True, vmem_limit_bytes=VMEM_BYTES if paired else 60 * 1024 * 1024
            ),
            name="newton_step",
        )(pattern, inverse_root, square_root)

    placed = P("layer", "rep", None, None)
    return jax.shard_map(
        body,
        mesh=mesh,
        in_specs=(placed, placed, P("layer", "rep")),
        out_specs=(placed, placed),
        check_vma=False,
    )
```

```python
import functools

import jax
import jax.numpy as jnp
from jax import lax
from jax.experimental import pallas as pl
from jax.experimental.pallas import tpu as pltpu
from jax.sharding import PartitionSpec as P

MESH = pl.DeviceIdType.MESH
VMEM = pl.BlockSpec(memory_space=pltpu.VMEM)
SMEM = pl.BlockSpec(memory_space=pltpu.SMEM)
SEMAPHORES = 256


def reached(rows, band, low, high):
    half = band // 2
    found = {1: {}, -1: {}}
    for i in range(rows):
        for u in range(band):
            j = i - half + u
            if 0 <= j < rows:
                continue
            assert -rows <= j < 2 * rows
            side, a = (1, j + rows) if j < 0 else (-1, j - rows)
            for w in range(low, high):
                v = w + half - u
                if 0 <= v < band:
                    lo, hi = found[side].get(a, (v, v + 1))
                    found[side][a] = (min(lo, v), max(hi, v + 1))
    return found


def rectangles(spans, first, last):
    cut = []
    for a in sorted(spans):
        lo, hi = max(spans[a][0], first), min(spans[a][1], last)
        if lo >= hi:
            continue
        if cut and cut[-1][1] == a and cut[-1][2:] == (lo, hi):
            cut[-1] = (cut[-1][0], a + 1, lo, hi)
        else:
            cut.append((a, a + 1, lo, hi))
    return cut


class Later:
    def __init__(self, make, args=None):
        self.make, self.args = make, args

    def __call__(self, *args):
        return Later(self.make, args)

    def start(self):
        self.make(*self.args).start()

    def wait_recv(self):
        self.make(*self.args).wait_recv()

    def wait_send(self):
        self.make(*self.args).wait_send()


def step_kernel(layers, reps, refs_shape, pattern, z_own, y_own, z_next, y_next, y_wide, z_wide, u_wide, send_sems, recv_sems):
    rows, slots, tile = refs_shape
    band = slots * reps
    half = band // 2
    layer, rep = lax.axis_index("layer"), lax.axis_index("rep")
    after, before = lax.rem(layer + 1, layers), lax.rem(layer + layers - 1, layers)
    may_send = {1: layer + 1 < layers, -1: layer > 0}
    may_take = {1: layer > 0, -1: layer + 1 < layers}
    bits = []
    bit = reps // 2
    while bit >= 2:
        bits.append(bit)
        bit //= 2
    masks = list(range(0, reps, 2))
    keys = {}
    wides = {"y": y_wide, "z": z_wide, "u": u_wide}
    relayed = ("z", "u") if reps == 4 else ()

    def keep(i, _):
        for w in range(slots):
            good = pattern[i, w] == 1
            for own, wide in ((y_own, y_wide), (z_own, z_wide)):
                part = own[i, w]
                wide[rows + i, rep * slots + w] = jnp.where(good, part, jnp.zeros_like(part))
        return 0

    lax.fori_loop(0, rows, keep, 0)

    barrier = pltpu.get_barrier_semaphore()
    for place in (after, before):
        pl.semaphore_signal(barrier, inc=1, device_id={"layer": place}, device_id_type=MESH)
    for flip in [1] + bits:
        partner = rep + flip * (1 - 2 * lax.rem(lax.div(rep, flip), 2))
        pl.semaphore_signal(barrier, inc=1, device_id={"rep": partner}, device_id_type=MESH)
    pl.semaphore_wait(barrier, 3 + len(bits))

    def schedule(me):
        chip = me // 2
        remote = []
        need = reached(rows, band, chip * 2 * slots, (chip + 1) * 2 * slots)
        union = reached(rows, band, 0, band)
        other = reached(rows, band, (1 - chip) * 2 * slots, (2 - chip) * 2 * slots) if relayed else None
        direct_side = 1 if chip == 0 else -1

        def spans(s, side):
            if s not in relayed:
                return need[side]
            return union[side] if side == direct_side else {}

        def arriving(s, side):
            return spans(s, side) or need[side]

        def cut(which, q):
            return rectangles(which, q * slots, (q + 1) * slots)

        def base(side):
            return 0 if side == 1 else 2 * rows

        def copy(key, src, dst, device):
            n = keys.setdefault(key, len(keys))
            return pltpu.make_async_remote_copy(
                src_ref=src, dst_ref=dst, send_sem=send_sems.at[n], recv_sem=recv_sems.at[n],
                device_id=device, device_id_type=MESH,
            )

        def begin(guard, made):
            remote.append((guard, made))
            if guard is None:
                made.start()
            else:
                pl.when(guard)(made.start)

        def shard(s, q):
            return wides[s].at[pl.ds(rows, rows), pl.ds(q * slots, slots)]

        @Later
        def across(s, m, bit):
            part = shard(s, me ^ bit ^ m)
            return copy(("y", s, m), part, part, {"rep": me ^ bit})

        @Later
        def across_in(s, m, bit):
            part = shard(s, me ^ m)
            return copy(("y", s, m), part, part, {"rep": me ^ bit})

        @Later
        def to_core(s, m):
            part = shard(s, me ^ m)
            return copy(("d", s, m), part, part, {"rep": me ^ 1})

        @Later
        def to_core_in(s, m):
            part = shard(s, me ^ 1 ^ m)
            return copy(("d", s, m), part, part, {"rep": me ^ 1})

        @Later
        def to_layer(s, side, m, k, piece):
            a, b, lo, hi = piece
            src = wides[s].at[pl.ds(rows + a, b - a), pl.ds(lo, hi - lo)]
            dst = wides[s].at[pl.ds(base(side) + a, b - a), pl.ds(lo, hi - lo)]
            return copy(("x", s, side, m, k), src, dst, {"layer": after if side == 1 else before})

        @Later
        def relay(s, side, m, k, piece):
            a, b, lo, hi = piece
            part = wides[s].at[pl.ds(base(side) + a, b - a), pl.ds(lo, hi - lo)]
            return copy(("r", s, side, m, k), part, part, {"rep": me ^ 2})

        @Later
        def halo_to_core(s, side, m, q):
            pieces = cut(arriving(s, side), q)
            a, b = min(c[0] for c in pieces), max(c[1] for c in pieces)
            part = wides[s].at[pl.ds(base(side) + a, b - a), pl.ds(q * slots, slots)]
            return copy(("h", s, side, m), part, part, {"rep": me ^ 1})

        def send_layer(s, m):
            for side in (1, -1):
                for k, piece in enumerate(cut(spans(s, side), me ^ m)):
                    begin(may_send[side], to_layer(s, side, m, k, piece))

        def take_direct(s, m):
            for side in (1, -1):
                pieces = cut(spans(s, side), me ^ m)
                if pieces:
                    made = [to_layer(s, side, m, k, piece) for k, piece in enumerate(pieces)]
                    onward = [halo_to_core(s, side, m, me ^ m)]
                    if s in relayed:
                        onward += [
                            relay(s, side, m ^ 2, k, piece)
                            for k, piece in enumerate(cut(other[side], me ^ m))
                        ]
                    pass_on(side, made, onward)

        def take_relayed(s, m):
            for side in (1, -1):
                if s in relayed and side != direct_side:
                    pieces = cut(need[side], me ^ m)
                    if pieces:
                        made = [relay(s, side, m, k, piece) for k, piece in enumerate(pieces)]
                        pass_on(side, made, [halo_to_core(s, side, m, me ^ m)])

        def pass_on(side, made, onward):
            remote.extend((may_take[side], o) for o in onward)

            @pl.when(may_take[side])
            def _():
                for one in made:
                    one.wait_recv()
                for one in onward:
                    one.start()

        def start_gather(s):
            if bits:
                begin(None, across(s, bits[0], bits[0]))
            begin(None, to_core(s, 0))

        def gather(s, halo):
            held = [0]
            for n, bit in enumerate(bits):
                if n > 0:
                    for m in held:
                        begin(None, across(s, m ^ bit, bit))
                fresh = [m ^ bit for m in held]
                for m in fresh:
                    across_in(s, m, bit).wait_recv()
                    begin(None, to_core(s, m))
                    if halo:
                        send_layer(s, m)
                held = held + fresh

        def finish_own(s):
            for m in masks:
                to_core_in(s, m).wait_recv()

        def finish_halo(s):
            for side in (1, -1):
                made = [
                    halo_to_core(s, side, m, me ^ 1 ^ m)
                    for m in masks
                    if cut(arriving(s, side), me ^ 1 ^ m)
                ]

                @pl.when(may_take[side])
                def _():
                    for one in made:
                        one.wait_recv()

        start_gather("y")
        start_gather("z")
        send_layer("y", 0)
        gather("y", True)
        send_layer("z", 0)
        take_direct("y", 0)
        gather("z", True)
        for m in masks[1:]:
            take_direct("y", m)
        for s in ("y", "z"):
            finish_own(s)
        finish_halo("y")
        yield
        start_gather("u")
        send_layer("u", 0)
        for m in masks:
            take_direct("z", m)
        gather("u", True)
        for m in masks:
            take_relayed("z", m)
        finish_own("u")
        finish_halo("z")
        yield
        for m in masks:
            take_direct("u", m)
        for m in masks:
            take_relayed("u", m)
        finish_halo("u")
        yield
        for guard, made in remote:
            if guard is None:
                made.wait_send()
            else:
                pl.when(guard)(made.wait_send)
        yield

    plans = [schedule(me) for me in range(reps)]

    def advance():
        for me in range(reps):
            pl.when(rep == me)(functools.partial(next, plans[me]))

    down = lax.broadcasted_iota(jnp.int32, (tile, tile), 0)
    right = lax.broadcasted_iota(jnp.int32, (tile, tile), 1)
    identity = jnp.where(down == right, 1.5, 0.0).astype(jnp.float32)

    def multiply(left, right, store):
        def step(i, _):
            total = product_row(i, left, right, layer, rep, layers, rows, slots, band)
            for w in range(slots):
                store(i, w, pattern[i, w] == 1, total[:, w * tile : (w + 1) * tile])
            return 0

        lax.fori_loop(0, rows, step, 0)

    def store_update(i, w, good, value):
        value = -0.5 * value + jnp.where(rep * slots + w == half, identity, 0.0)
        u_wide[rows + i, rep * slots + w] = jnp.where(good, value, 0.0).astype(jnp.bfloat16)

    def store_inverse(i, w, good, value):
        z_next[i, w] = jnp.where(good, value, 0.0).astype(jnp.bfloat16)

    def store_square(i, w, good, value):
        y_next[i, w] = jnp.where(good, value, 0.0).astype(jnp.bfloat16)

    advance()
    multiply(z_wide, y_wide, store_update)
    advance()
    multiply(u_wide, z_wide, store_inverse)
    advance()
    multiply(y_wide, u_wide, store_square)
    advance()
    assert len(keys) <= send_sems.shape[0]


def product_row(i, left, right, layer, rep, layers, rows, slots, band):
    half = band // 2
    step = 4
    total = None
    for first in range(0, band, step):
        wide = jnp.concatenate([left[rows + i, u] for u in range(first, first + step)], axis=1)
        tall = []
        for u in range(first, first + step):
            row = layer * rows + i - half + u
            inside = jnp.logical_and(row >= 0, row < layers * rows)
            tiles = []
            for w in range(slots):
                v = rep * slots + w + half - u
                good = jnp.logical_and(inside, jnp.logical_and(v >= 0, v < band))
                part = right[i + u + rows - half, lax.rem(v + band, band)]
                tiles.append(jnp.where(good, part, jnp.zeros_like(part)))
            tall.append(jnp.concatenate(tiles, axis=1))
        piece = jnp.dot(wide, jnp.concatenate(tall, axis=0), preferred_element_type=jnp.float32)
        total = piece if total is None else total + piece
    return total


PAIRED_SEMAPHORES = 144
VMEM_BYTES = 50 * 1024 * 1024


def block_spans(rows, band):
    lower = {a: (0, band // 2 - a) for a in range(rows)}
    upper = {a: (band - a, band) for a in range(1, rows)}
    return lower, upper


def paired_kernel(
    layers, reps, refs_shape, pattern, z_own, y_own, z_next, y_next,
    y_wide, z_wide, u_wide, z_sum, y_sum, c_out, z_out, y_out, c_in, z_in, y_in, send_sems, recv_sems,
):
    rows, slots, tile = refs_shape
    band = slots * reps
    half = band // 2
    step = 2
    chunks = [(a, a + step) for a in range(0, rows, step)]
    layer, rep = lax.axis_index("layer"), lax.axis_index("rep")
    after, before = lax.rem(layer + 1, layers), lax.rem(layer + layers - 1, layers)
    may_send = {1: layer + 1 < layers, -1: layer > 0}
    may_take = {1: layer > 0, -1: layer + 1 < layers}
    wides = {"y": y_wide, "z": z_wide, "u": u_wide}
    partials = {"c": (c_out, c_in), "z": (z_out, z_in), "y": (y_out, y_in)}
    lower, upper = block_spans(rows, band)
    keys = {}

    barrier = pltpu.get_barrier_semaphore()
    for place in (after, before):
        pl.semaphore_signal(barrier, inc=1, device_id={"layer": place}, device_id_type=MESH)
    for flip in (1, 2):
        partner = rep + flip * (1 - 2 * lax.rem(lax.div(rep, flip), 2))
        pl.semaphore_signal(barrier, inc=1, device_id={"rep": partner}, device_id_type=MESH)

    def keep(own, wide):
        def row(i, _):
            for w in range(slots):
                part = own[i, w]
                wide[rows + i, rep * slots + w] = jnp.where(pattern[i, w] == 1, part, jnp.zeros_like(part))
            return 0

        lax.fori_loop(0, rows, row, 0)

    class Parcel:
        def __init__(self, n, pairs, device):
            self.n, self.pairs, self.device = n, pairs, device

        def copies(self):
            for src, dst in self.pairs:
                yield pltpu.make_async_remote_copy(
                    src_ref=src, dst_ref=dst, send_sem=send_sems.at[0], recv_sem=recv_sems.at[self.n],
                    device_id=self.device, device_id_type=MESH,
                )

        def start(self):
            for one in self.copies():
                one.start()

        def wait_send(self):
            for one in self.copies():
                one.wait_send()

        def wait_recv(self):
            if len(self.pairs) == 1:
                next(self.copies()).wait_recv()
                return
            tiles = sum(dst.shape[0] * dst.shape[1] for _, dst in self.pairs)
            at = y_wide.at[pl.ds(0, 1), pl.ds(0, tiles)]
            Parcel(self.n, [(at, at)], self.device).wait_recv()

    def schedule(me):
        chip = me // 2
        remote = []

        def base(side):
            return 0 if side == 1 else 2 * rows

        def own_side(who):
            return -1 if who // 2 == 0 else 1

        def own_spans(who):
            return lower if who // 2 == 0 else upper

        def cut(spans, q, chunk):
            kept = {a: spans[a] for a in spans if chunk[0] <= a < chunk[1]}
            return rectangles(kept, q * slots, (q + 1) * slots)

        def needs(who, side):
            low = who // 2 * 2 * slots
            return reached(rows, band, low, low + 2 * slots)[side]

        def sent(s, who, side, n):
            if side == own_side(who):
                return {} if n else own_spans(who)
            return shared(who ^ 2) if n and s == "y" else {}

        def shared(who):
            side = own_side(who)
            need, have = needs(who ^ 2, side), own_spans(who)
            found = {}
            for a in have:
                if a in need:
                    lo, hi = max(need[a][0], have[a][0]), min(need[a][1], have[a][1])
                    if lo < hi:
                        found[a] = (lo, hi)
            return found

        def copy(key, src, dst, device):
            return Parcel(keys.setdefault(key, len(keys)), [(src, dst)], device)

        def begin(guard, made):
            if not made:
                return
            remote.append((guard, made))

            def go():
                for one in made:
                    one.start()

            go() if guard is None else pl.when(guard)(go)

        def take(guard, made, onward=()):
            if not made:
                return
            remote.append((guard, list(onward)))

            def go():
                for one in made:
                    one.wait_recv()
                for one in onward:
                    one.start()

            go() if guard is None else pl.when(guard)(go)

        def shard(s, q, chunk):
            return wides[s].at[pl.ds(rows + chunk[0], chunk[1] - chunk[0]), pl.ds(q * slots, slots)]

        def swap(s, q, chunk):
            part = shard(s, q, chunk)
            return copy(("swap", s, chunk), part, part, {"rep": me ^ 2})

        def pair(s, q, chunk):
            part = shard(s, q, chunk)
            return copy(("pair", s, chunk), part, part, {"rep": me ^ 1})

        def pass_pair(s, q, chunk):
            part = shard(s, q, chunk)
            return copy(("pass", s, chunk), part, part, {"rep": me ^ 1})

        def parcel(key, pairs, device):
            return [Parcel(keys.setdefault(key, len(keys)), pairs, device)] if pairs else []

        def boxes(name, s, side, n, chunk, pieces, device, start):
            pairs = []
            for a, b, lo, hi in pieces:
                src = wides[s].at[pl.ds(start + a, b - a), pl.ds(lo, hi - lo)]
                dst = wides[s].at[pl.ds(base(side) + a, b - a), pl.ds(lo, hi - lo)]
                pairs.append((src, dst))
            return parcel((name, s, side, n, chunk), pairs, device)

        def group(who, n):
            return who ^ 2 if n else who

        def to_layer(s, side, n, chunk):
            pieces = cut(sent(s, me, side, n), group(me, n), chunk)
            return boxes("x", s, side, n, chunk, pieces, {"layer": after if side == 1 else before}, rows)

        def layer_pass(s, side, n, chunk, who):
            pieces = cut(sent(s, who, side, n), group(who, n), chunk)
            return boxes("xp", s, side, n, chunk, pieces, {"rep": me ^ 1}, base(side))

        def relay(s, chunk, who):
            pieces = cut(shared(who), who, chunk)
            side = own_side(who)
            return boxes("r", s, side, 0, chunk, pieces, {"rep": me ^ 2}, base(side))

        def relay_pass(s, chunk, who):
            pieces = cut(shared(who), who, chunk)
            side = own_side(who)
            return boxes("rp", s, side, 0, chunk, pieces, {"rep": me ^ 1}, base(side))

        def partial_out(s, chunk):
            source, target = partials[s]
            pairs = []
            for a, b, lo, hi in cut(own_spans(me), me, chunk):
                at = (pl.ds(a, b - a), pl.ds(lo - me * slots, hi - lo))
                pairs.append((source.at[at], target.at[at]))
            return parcel(("p", s, chunk), pairs, {"layer": after if chip == 0 else before})

        def start_swap(s, chunk):
            begin(None, [swap(s, me, chunk)])

        def start_pair(s, chunk):
            begin(None, [pair(s, me, chunk)])

        def end_swap(s, chunk):
            take(None, [swap(s, me ^ 2, chunk)], [pass_pair(s, me ^ 2, chunk)])

        def send_layer(s, n, chunk):
            for side in (1, -1):
                begin(may_send[side], to_layer(s, side, n, chunk))

        def take_layer(s, n, chunk):
            for side in (1, -1):
                take(may_take[side], to_layer(s, side, n, chunk), layer_pass(s, side, n, chunk, me))

        def take_layer_pass(s, n, chunk):
            for side in (1, -1):
                take(may_take[side], layer_pass(s, side, n, chunk, me ^ 1))

        def take_relay(s, chunk):
            take(may_take[own_side(me ^ 2)], relay(s, chunk, me ^ 2), relay_pass(s, chunk, me ^ 2))

        def take_relay_pass(s, chunk):
            take(may_take[own_side(me ^ 2)], relay_pass(s, chunk, me ^ 3))

        out_side = 1 if chip == 0 else -1

        for chunk in chunks:
            start_swap("y", chunk)
        yield
        for s in ("z", "y"):
            for chunk in chunks:
                send_layer(s, 0, chunk)
        for chunk in chunks:
            start_swap("z", chunk)
        for s in ("y", "z"):
            for chunk in chunks:
                start_pair(s, chunk)
        for chunk in chunks:
            end_swap("y", chunk)
            send_layer("y", 1, chunk)
        for chunk in chunks:
            take_layer("z", 0, chunk)
        for chunk in chunks:
            take(None, [pair("y", me ^ 1, chunk)])
            take(None, [pass_pair("y", me ^ 3, chunk)])
            take_layer_pass("z", 0, chunk)
        yield
        for chunk in chunks:
            begin(may_send[out_side], partial_out("c", chunk))
        for n, chunk in enumerate(chunks[:-1]):
            end_swap("z", chunk)
            take_layer("y", 1, chunk)
            take(None, [pair("z", me ^ 1, chunk)])
            if n:
                take(None, [pass_pair("z", me ^ 3, chunks[n - 1])])
                yield
        take_layer("y", 1, chunks[-1])
        for chunk in chunks:
            if chip == 1:
                take_layer("y", 0, chunk)
            take_layer_pass("y", 1, chunk)
        if chip == 1:
            for chunk in chunks:
                take_layer_pass("y", 0, chunk)
        take(None, [pair("z", me ^ 1, chunks[-1])])
        take(None, [pass_pair("z", me ^ 3, chunks[-2])])
        for chunk in chunks:
            if chunk == chunks[1]:
                end_swap("z", chunks[-1])
            if chunk == chunks[-1]:
                take(None, [pass_pair("z", me ^ 3, chunk)])
            if chip == 0:
                take_layer("y", 0, chunk)
                take_layer_pass("y", 0, chunk)
            take(may_take[out_side], partial_out("c", chunk))
            yield
            start_swap("u", chunk)
            start_pair("u", chunk)
            if chunk == chunks[-2]:
                for one in chunks[:-1]:
                    send_layer("u", 0, one)
        send_layer("u", 0, chunks[-1])
        for chunk in chunks:
            begin(may_take[own_side(me)], relay("z", chunk, me))
        first, last = chunks[: len(chunks) // 2], chunks[len(chunks) // 2 :]
        for some in (first, last):
            for chunk in some:
                if chunk != chunks[-1]:
                    end_swap("u", chunk)
                take_layer("u", 0, chunk)
            for chunk in some:
                take_layer_pass("u", 0, chunk)
            yield
        for chunk in chunks:
            begin(may_send[out_side], partial_out("z", chunk))
        for chunk in chunks[:: 1 if chip == 0 else -1]:
            begin(may_take[own_side(me)], relay("u", chunk, me))
        for chunk in chunks:
            if chunk == chunks[-1]:
                end_swap("u", chunk)
            take(None, [pair("u", me ^ 1, chunk)])
            take(None, [pass_pair("u", me ^ 3, chunk)])
        yield
        for chunk in chunks:
            begin(may_send[out_side], partial_out("y", chunk))
        yield
        for chunk in chunks:
            take_relay("z", chunk)
        yield
        for chunk in chunks:
            take_relay_pass("z", chunk)
        yield
        arriving = chunks[:: 1 if chip == 1 else -1]
        for chunk in arriving[:-1]:
            take_relay("u", chunk)
        for n, chunk in enumerate(arriving):
            if n == len(arriving) - 2:
                take_relay("u", arriving[-1])
            take_relay_pass("u", chunk)
            yield
        for chunk in chunks:
            take(may_take[out_side], partial_out("z", chunk))
        yield
        for chunk in chunks:
            take(may_take[out_side], partial_out("y", chunk))
        yield
        for guard, made in remote:

            def end(made=made):
                for one in made:
                    one.wait_send()

            if made:
                end() if guard is None else pl.when(guard)(end)
        yield

    plans = [schedule(me) for me in range(reps)]

    def advance():
        for me in range(reps):
            pl.when(rep == me)(functools.partial(next, plans[me]))

    down = lax.broadcasted_iota(jnp.int32, (tile, tile), 0)
    right_at = lax.broadcasted_iota(jnp.int32, (tile, tile), 1)
    identity = jnp.where(down == right_at, 1.5, 0.0).astype(jnp.float32)
    zero = jnp.zeros((tile, tile), jnp.bfloat16)

    def multiply(lefts, rights):
        wide = jnp.concatenate(lefts, axis=1)
        tall = jnp.concatenate([jnp.concatenate(one, axis=1) for one in rights], axis=0)
        return jnp.dot(wide, tall, preferred_element_type=jnp.float32)

    def own_part(i, left, right):
        lefts, rights = [], []
        for t in range(rows):
            u = half - i + t
            lefts.append(left[rows + i, u])
            line = []
            for w in range(slots):
                v = rep * slots + w + i - t
                good = jnp.logical_and(v >= 0, v < band)
                line.append(jnp.where(good, right[rows + t, lax.rem(v + band, band)], zero))
            rights.append(line)
        return multiply(lefts, rights)

    def halo_part(i, left, right):
        lefts, rights = [], []
        for t in range(rows):
            u = lax.rem(t - i + band, band)
            lefts.append(left[rows + i, u])
            line = []
            row = layer * rows + i - half + u
            inside = jnp.logical_and(row >= 0, row < layers * rows)
            for w in range(slots):
                v = rep * slots + w + half - u
                good = jnp.logical_and(inside, jnp.logical_and(v >= 0, v < band))
                k = i - half + rep * slots + w
                good = jnp.logical_and(good, jnp.logical_and(k >= 0, k < rows))
                line.append(jnp.where(good, right[i + u, lax.rem(v + band, band)], zero))
            rights.append(line)
        return multiply(lefts, rights)

    def split(total, w):
        return total[:, w * tile : (w + 1) * tile]

    def returned(part, i, w):
        k = i - half + rep * slots + w
        below = jnp.logical_and(k < 0, layer > 0)
        above = jnp.logical_and(k >= rows, layer + 1 < layers)
        return jnp.where(jnp.logical_or(below, above), part[i, w].astype(jnp.float32), 0.0)

    def update_rows(chunk):
        def row(i, _):
            total = halo_part(i, z_wide, y_wide)
            for w in range(slots):
                value = -0.5 * (split(total, w) + z_sum[i, w] + returned(c_in, i, w))
                value += jnp.where(rep * slots + w == half, identity, 0.0)
                value = jnp.where(pattern[i, w] == 1, value, 0.0)
                u_wide[rows + i, rep * slots + w] = value.astype(jnp.bfloat16)
            return 0

        lax.fori_loop(chunk[0], chunk[1], row, 0)

    def own_rows(left, right, total, chunk):
        def row(i, _):
            value = own_part(i, left, right)
            for w in range(slots):
                total[i, w] = split(value, w)
            return 0

        lax.fori_loop(chunk[0], chunk[1], row, 0)

    def halo_rows(left, right, total, n, turn):
        def row(r, _):
            i = n * step + r
            if turn:
                i = lax.div(rep, 2) * (2 * n * step + step - rows) + rows - step - n * step + r
            value = halo_part(i, left, right)
            for w in range(slots):
                total[i, w] += split(value, w)
            return 0

        lax.fori_loop(0, step if turn else rows, row, 0)

    def partial_rows(left, right, out, chunk):
        chip = lax.div(rep, 2)

        def row(i, _):
            lefts, rights = [], []
            for t in range(rows):
                u = t + half * chip
                part = left[2 * rows * (1 - chip) + i, u]
                lefts.append(jnp.where(lax.div(i + t, rows) == chip, part, zero))
                j = lax.rem(i + t, rows)
                rights.append([
                    right[rows + j, rep * slots + w + half - u] for w in range(slots)
                ])
            value = multiply(lefts, rights)
            for w in range(slots):
                out[i, w] = split(value, w).astype(jnp.bfloat16)
            return 0

        lax.fori_loop(chunk[0], chunk[1], row, 0)

    def finish(total, part, result):
        def row(i, _):
            for w in range(slots):
                value = jnp.where(pattern[i, w] == 1, total[i, w] + returned(part, i, w), 0.0)
                result[i, w] = value.astype(jnp.bfloat16)
            return 0

        lax.fori_loop(0, rows, row, 0)

    keep(y_own, y_wide)
    pl.semaphore_wait(barrier, 4)
    advance()
    keep(z_own, z_wide)
    middle = rows // 2
    advance()
    partial_rows(z_wide, y_wide, c_out, (0, rows))
    for chunk in chunks[:-2]:
        advance()
        own_rows(z_wide, y_wide, z_sum, chunk)
    for chunk in chunks:
        advance()
        if chunk == chunks[0]:
            own_rows(z_wide, y_wide, z_sum, chunks[-2])
        if chunk == chunks[-1]:
            own_rows(z_wide, y_wide, z_sum, chunk)
        update_rows(chunk)
    for chunk in ((0, middle), (middle, rows)):
        advance()
        partial_rows(u_wide, z_wide, z_out, chunk)
    advance()
    partial_rows(y_wide, u_wide, y_out, (0, rows))
    advance()
    own_rows(u_wide, z_wide, z_sum, (0, rows))
    advance()
    own_rows(y_wide, u_wide, y_sum, (0, rows))
    advance()
    halo_rows(u_wide, z_wide, z_sum, 0, False)
    for n in range(len(chunks)):
        advance()
        halo_rows(y_wide, u_wide, y_sum, n, True)
    advance()
    finish(z_sum, z_in, z_next)
    advance()
    finish(y_sum, y_in, y_next)
    advance()
    assert len(keys) <= recv_sems.shape[0]


def solution(mesh):
    layers, reps = mesh.shape["layer"], mesh.shape["rep"]

    def body(inverse_root, square_root, pattern):
        rows, slots = pattern.shape
        tile = inverse_root.shape[2:]
        local = jax.ShapeDtypeStruct((rows, slots) + tile, jnp.bfloat16)
        wide = pltpu.VMEM((3 * rows, slots * reps) + tile, jnp.bfloat16)
        sems = [pltpu.SemaphoreType.DMA((SEMAPHORES,))] * 2
        paired = reps == 4 and 2 * rows == slots * reps and rows % 4 == 0
        kernel, extra = step_kernel, []
        if paired:
            kernel = paired_kernel
            extra = [pltpu.VMEM((rows, slots) + tile, jnp.float32)] * 2
            extra += [pltpu.VMEM((rows, slots) + tile, jnp.bfloat16)] * 6
            sems = [pltpu.SemaphoreType.DMA((1,)), pltpu.SemaphoreType.DMA((PAIRED_SEMAPHORES,))]
        return pl.pallas_call(
            functools.partial(kernel, layers, reps, (rows, slots, tile[0])),
            out_shape=(local, local),
            in_specs=[SMEM, VMEM, VMEM],
            out_specs=(VMEM, VMEM),
            scratch_shapes=[wide, wide, wide] + extra + sems,
            compiler_params=pltpu.CompilerParams(
                collective_id=0, has_side_effects=True, vmem_limit_bytes=VMEM_BYTES if paired else 60 * 1024 * 1024
            ),
            name="newton_step",
        )(pattern, inverse_root, square_root)

    placed = P("layer", "rep", None, None)
    return jax.shard_map(
        body,
        mesh=mesh,
        in_specs=(placed, placed, P("layer", "rep")),
        out_specs=(placed, placed),
        check_vma=False,
    )
```

```python
import functools

import jax
import jax.numpy as jnp
from jax import lax
from jax.experimental import pallas as pl
from jax.experimental.pallas import tpu as pltpu
from jax.sharding import PartitionSpec as P

MESH = pl.DeviceIdType.MESH
VMEM = pl.BlockSpec(memory_space=pltpu.VMEM)
SMEM = pl.BlockSpec(memory_space=pltpu.SMEM)
SEMAPHORES = 256


def reached(rows, band, low, high):
    half = band // 2
    found = {1: {}, -1: {}}
    for i in range(rows):
        for u in range(band):
            j = i - half + u
            if 0 <= j < rows:
                continue
            assert -rows <= j < 2 * rows
            side, a = (1, j + rows) if j < 0 else (-1, j - rows)
            for w in range(low, high):
                v = w + half - u
                if 0 <= v < band:
                    lo, hi = found[side].get(a, (v, v + 1))
                    found[side][a] = (min(lo, v), max(hi, v + 1))
    return found


def rectangles(spans, first, last):
    cut = []
    for a in sorted(spans):
        lo, hi = max(spans[a][0], first), min(spans[a][1], last)
        if lo >= hi:
            continue
        if cut and cut[-1][1] == a and cut[-1][2:] == (lo, hi):
            cut[-1] = (cut[-1][0], a + 1, lo, hi)
        else:
            cut.append((a, a + 1, lo, hi))
    return cut


class Later:
    def __init__(self, make, args=None):
        self.make, self.args = make, args

    def __call__(self, *args):
        return Later(self.make, args)

    def start(self):
        self.make(*self.args).start()

    def wait_recv(self):
        self.make(*self.args).wait_recv()

    def wait_send(self):
        self.make(*self.args).wait_send()


def step_kernel(layers, reps, refs_shape, pattern, z_own, y_own, z_next, y_next, y_wide, z_wide, u_wide, send_sems, recv_sems):
    rows, slots, tile = refs_shape
    band = slots * reps
    half = band // 2
    layer, rep = lax.axis_index("layer"), lax.axis_index("rep")
    after, before = lax.rem(layer + 1, layers), lax.rem(layer + layers - 1, layers)
    may_send = {1: layer + 1 < layers, -1: layer > 0}
    may_take = {1: layer > 0, -1: layer + 1 < layers}
    bits = []
    bit = reps // 2
    while bit >= 2:
        bits.append(bit)
        bit //= 2
    masks = list(range(0, reps, 2))
    keys = {}
    wides = {"y": y_wide, "z": z_wide, "u": u_wide}
    relayed = ("z", "u") if reps == 4 else ()

    def keep(i, _):
        for w in range(slots):
            good = pattern[i, w] == 1
            for own, wide in ((y_own, y_wide), (z_own, z_wide)):
                part = own[i, w]
                wide[rows + i, rep * slots + w] = jnp.where(good, part, jnp.zeros_like(part))
        return 0

    lax.fori_loop(0, rows, keep, 0)

    barrier = pltpu.get_barrier_semaphore()
    for place in (after, before):
        pl.semaphore_signal(barrier, inc=1, device_id={"layer": place}, device_id_type=MESH)
    for flip in [1] + bits:
        partner = rep + flip * (1 - 2 * lax.rem(lax.div(rep, flip), 2))
        pl.semaphore_signal(barrier, inc=1, device_id={"rep": partner}, device_id_type=MESH)
    pl.semaphore_wait(barrier, 3 + len(bits))

    def schedule(me):
        chip = me // 2
        remote = []
        need = reached(rows, band, chip * 2 * slots, (chip + 1) * 2 * slots)
        union = reached(rows, band, 0, band)
        other = reached(rows, band, (1 - chip) * 2 * slots, (2 - chip) * 2 * slots) if relayed else None
        direct_side = 1 if chip == 0 else -1

        def spans(s, side):
            if s not in relayed:
                return need[side]
            return union[side] if side == direct_side else {}

        def arriving(s, side):
            return spans(s, side) or need[side]

        def cut(which, q):
            return rectangles(which, q * slots, (q + 1) * slots)

        def base(side):
            return 0 if side == 1 else 2 * rows

        def copy(key, src, dst, device):
            n = keys.setdefault(key, len(keys))
            return pltpu.make_async_remote_copy(
                src_ref=src, dst_ref=dst, send_sem=send_sems.at[n], recv_sem=recv_sems.at[n],
                device_id=device, device_id_type=MESH,
            )

        def begin(guard, made):
            remote.append((guard, made))
            if guard is None:
                made.start()
            else:
                pl.when(guard)(made.start)

        def shard(s, q):
            return wides[s].at[pl.ds(rows, rows), pl.ds(q * slots, slots)]

        @Later
        def across(s, m, bit):
            part = shard(s, me ^ bit ^ m)
            return copy(("y", s, m), part, part, {"rep": me ^ bit})

        @Later
        def across_in(s, m, bit):
            part = shard(s, me ^ m)
            return copy(("y", s, m), part, part, {"rep": me ^ bit})

        @Later
        def to_core(s, m):
            part = shard(s, me ^ m)
            return copy(("d", s, m), part, part, {"rep": me ^ 1})

        @Later
        def to_core_in(s, m):
            part = shard(s, me ^ 1 ^ m)
            return copy(("d", s, m), part, part, {"rep": me ^ 1})

        @Later
        def to_layer(s, side, m, k, piece):
            a, b, lo, hi = piece
            src = wides[s].at[pl.ds(rows + a, b - a), pl.ds(lo, hi - lo)]
            dst = wides[s].at[pl.ds(base(side) + a, b - a), pl.ds(lo, hi - lo)]
            return copy(("x", s, side, m, k), src, dst, {"layer": after if side == 1 else before})

        @Later
        def relay(s, side, m, k, piece):
            a, b, lo, hi = piece
            part = wides[s].at[pl.ds(base(side) + a, b - a), pl.ds(lo, hi - lo)]
            return copy(("r", s, side, m, k), part, part, {"rep": me ^ 2})

        @Later
        def halo_to_core(s, side, m, q):
            pieces = cut(arriving(s, side), q)
            a, b = min(c[0] for c in pieces), max(c[1] for c in pieces)
            part = wides[s].at[pl.ds(base(side) + a, b - a), pl.ds(q * slots, slots)]
            return copy(("h", s, side, m), part, part, {"rep": me ^ 1})

        def send_layer(s, m):
            for side in (1, -1):
                for k, piece in enumerate(cut(spans(s, side), me ^ m)):
                    begin(may_send[side], to_layer(s, side, m, k, piece))

        def take_direct(s, m):
            for side in (1, -1):
                pieces = cut(spans(s, side), me ^ m)
                if pieces:
                    made = [to_layer(s, side, m, k, piece) for k, piece in enumerate(pieces)]
                    onward = [halo_to_core(s, side, m, me ^ m)]
                    if s in relayed:
                        onward += [
                            relay(s, side, m ^ 2, k, piece)
                            for k, piece in enumerate(cut(other[side], me ^ m))
                        ]
                    pass_on(side, made, onward)

        def take_relayed(s, m):
            for side in (1, -1):
                if s in relayed and side != direct_side:
                    pieces = cut(need[side], me ^ m)
                    if pieces:
                        made = [relay(s, side, m, k, piece) for k, piece in enumerate(pieces)]
                        pass_on(side, made, [halo_to_core(s, side, m, me ^ m)])

        def pass_on(side, made, onward):
            remote.extend((may_take[side], o) for o in onward)

            @pl.when(may_take[side])
            def _():
                for one in made:
                    one.wait_recv()
                for one in onward:
                    one.start()

        def start_gather(s):
            if bits:
                begin(None, across(s, bits[0], bits[0]))
            begin(None, to_core(s, 0))

        def gather(s, halo):
            held = [0]
            for n, bit in enumerate(bits):
                if n > 0:
                    for m in held:
                        begin(None, across(s, m ^ bit, bit))
                fresh = [m ^ bit for m in held]
                for m in fresh:
                    across_in(s, m, bit).wait_recv()
                    begin(None, to_core(s, m))
                    if halo:
                        send_layer(s, m)
                held = held + fresh

        def finish_own(s):
            for m in masks:
                to_core_in(s, m).wait_recv()

        def finish_halo(s):
            for side in (1, -1):
                made = [
                    halo_to_core(s, side, m, me ^ 1 ^ m)
                    for m in masks
                    if cut(arriving(s, side), me ^ 1 ^ m)
                ]

                @pl.when(may_take[side])
                def _():
                    for one in made:
                        one.wait_recv()

        start_gather("y")
        start_gather("z")
        send_layer("y", 0)
        gather("y", True)
        send_layer("z", 0)
        take_direct("y", 0)
        gather("z", True)
        for m in masks[1:]:
            take_direct("y", m)
        for s in ("y", "z"):
            finish_own(s)
        finish_halo("y")
        yield
        start_gather("u")
        send_layer("u", 0)
        for m in masks:
            take_direct("z", m)
        gather("u", True)
        for m in masks:
            take_relayed("z", m)
        finish_own("u")
        finish_halo("z")
        yield
        for m in masks:
            take_direct("u", m)
        for m in masks:
            take_relayed("u", m)
        finish_halo("u")
        yield
        for guard, made in remote:
            if guard is None:
                made.wait_send()
            else:
                pl.when(guard)(made.wait_send)
        yield

    plans = [schedule(me) for me in range(reps)]

    def advance():
        for me in range(reps):
            pl.when(rep == me)(functools.partial(next, plans[me]))

    down = lax.broadcasted_iota(jnp.int32, (tile, tile), 0)
    right = lax.broadcasted_iota(jnp.int32, (tile, tile), 1)
    identity = jnp.where(down == right, 1.5, 0.0).astype(jnp.float32)

    def multiply(left, right, store):
        def step(i, _):
            total = product_row(i, left, right, layer, rep, layers, rows, slots, band)
            for w in range(slots):
                store(i, w, pattern[i, w] == 1, total[:, w * tile : (w + 1) * tile])
            return 0

        lax.fori_loop(0, rows, step, 0)

    def store_update(i, w, good, value):
        value = -0.5 * value + jnp.where(rep * slots + w == half, identity, 0.0)
        u_wide[rows + i, rep * slots + w] = jnp.where(good, value, 0.0).astype(jnp.bfloat16)

    def store_inverse(i, w, good, value):
        z_next[i, w] = jnp.where(good, value, 0.0).astype(jnp.bfloat16)

    def store_square(i, w, good, value):
        y_next[i, w] = jnp.where(good, value, 0.0).astype(jnp.bfloat16)

    advance()
    multiply(z_wide, y_wide, store_update)
    advance()
    multiply(u_wide, z_wide, store_inverse)
    advance()
    multiply(y_wide, u_wide, store_square)
    advance()
    assert len(keys) <= send_sems.shape[0]


def product_row(i, left, right, layer, rep, layers, rows, slots, band):
    half = band // 2
    step = 4
    total = None
    for first in range(0, band, step):
        wide = jnp.concatenate([left[rows + i, u] for u in range(first, first + step)], axis=1)
        tall = []
        for u in range(first, first + step):
            row = layer * rows + i - half + u
            inside = jnp.logical_and(row >= 0, row < layers * rows)
            tiles = []
            for w in range(slots):
                v = rep * slots + w + half - u
                good = jnp.logical_and(inside, jnp.logical_and(v >= 0, v < band))
                part = right[i + u + rows - half, lax.rem(v + band, band)]
                tiles.append(jnp.where(good, part, jnp.zeros_like(part)))
            tall.append(jnp.concatenate(tiles, axis=1))
        piece = jnp.dot(wide, jnp.concatenate(tall, axis=0), preferred_element_type=jnp.float32)
        total = piece if total is None else total + piece
    return total


PAIRED_SEMAPHORES = 152
VMEM_BYTES = 50 * 1024 * 1024


def block_spans(rows, band):
    lower = {a: (0, band // 2 - a) for a in range(rows)}
    upper = {a: (band - a, band) for a in range(1, rows)}
    return lower, upper


def paired_kernel(
    layers, reps, refs_shape, pattern, z_own, y_own, z_next, y_next,
    y_wide, z_wide, u_wide, z_sum, y_sum, c_out, z_out, y_out, c_in, z_in, y_in, send_sems, recv_sems,
):
    rows, slots, tile = refs_shape
    band = slots * reps
    half = band // 2
    step = 2
    chunks = [(a, a + step) for a in range(0, rows, step)]
    layer, rep = lax.axis_index("layer"), lax.axis_index("rep")
    after, before = lax.rem(layer + 1, layers), lax.rem(layer + layers - 1, layers)
    may_send = {1: layer + 1 < layers, -1: layer > 0}
    may_take = {1: layer > 0, -1: layer + 1 < layers}
    wides = {"y": y_wide, "z": z_wide, "u": u_wide}
    partials = {"c": (c_out, c_in), "z": (z_out, z_in), "y": (y_out, y_in)}
    lower, upper = block_spans(rows, band)
    keys = {}

    barrier = pltpu.get_barrier_semaphore()
    for place in (after, before):
        pl.semaphore_signal(barrier, inc=1, device_id={"layer": place}, device_id_type=MESH)
    for flip in (1, 2):
        partner = rep + flip * (1 - 2 * lax.rem(lax.div(rep, flip), 2))
        pl.semaphore_signal(barrier, inc=1, device_id={"rep": partner}, device_id_type=MESH)

    def keep(own, wide):
        def row(i, _):
            for w in range(slots):
                part = own[i, w]
                wide[rows + i, rep * slots + w] = jnp.where(pattern[i, w] == 1, part, jnp.zeros_like(part))
            return 0

        lax.fori_loop(0, rows, row, 0)

    class Parcel:
        def __init__(self, n, pairs, device):
            self.n, self.pairs, self.device = n, pairs, device

        def copies(self):
            for src, dst in self.pairs:
                yield pltpu.make_async_remote_copy(
                    src_ref=src, dst_ref=dst, send_sem=send_sems.at[0], recv_sem=recv_sems.at[self.n],
                    device_id=self.device, device_id_type=MESH,
                )

        def start(self):
            for one in self.copies():
                one.start()

        def wait_send(self):
            for one in self.copies():
                one.wait_send()

        def wait_recv(self):
            if len(self.pairs) == 1:
                next(self.copies()).wait_recv()
                return
            tiles = sum(dst.shape[0] * dst.shape[1] for _, dst in self.pairs)
            at = y_wide.at[pl.ds(0, 1), pl.ds(0, tiles)]
            Parcel(self.n, [(at, at)], self.device).wait_recv()

    def schedule(me):
        chip = me // 2
        remote = []

        def base(side):
            return 0 if side == 1 else 2 * rows

        def own_side(who):
            return -1 if who // 2 == 0 else 1

        def own_spans(who):
            return lower if who // 2 == 0 else upper

        def cut(spans, q, chunk):
            kept = {a: spans[a] for a in spans if chunk[0] <= a < chunk[1]}
            return rectangles(kept, q * slots, (q + 1) * slots)

        def needs(who, side):
            low = who // 2 * 2 * slots
            return reached(rows, band, low, low + 2 * slots)[side]

        def sent(s, who, side, n):
            if side == own_side(who):
                return {} if n else own_spans(who)
            return shared(who ^ 2) if n and (s == "y" or s == "z" and who // 2) else {}

        def shared(who):
            side = own_side(who)
            need, have = needs(who ^ 2, side), own_spans(who)
            found = {}
            for a in have:
                if a in need:
                    lo, hi = max(need[a][0], have[a][0]), min(need[a][1], have[a][1])
                    if lo < hi:
                        found[a] = (lo, hi)
            return found

        def copy(key, src, dst, device):
            return Parcel(keys.setdefault(key, len(keys)), [(src, dst)], device)

        def begin(guard, made):
            if not made:
                return
            remote.append((guard, made))

            def go():
                for one in made:
                    one.start()

            go() if guard is None else pl.when(guard)(go)

        def take(guard, made, onward=()):
            if not made:
                return
            remote.append((guard, list(onward)))

            def go():
                for one in made:
                    one.wait_recv()
                for one in onward:
                    one.start()

            go() if guard is None else pl.when(guard)(go)

        def shard(s, q, chunk):
            return wides[s].at[pl.ds(rows + chunk[0], chunk[1] - chunk[0]), pl.ds(q * slots, slots)]

        def swap(s, q, chunk):
            part = shard(s, q, chunk)
            return copy(("swap", s, chunk), part, part, {"rep": me ^ 2})

        def pair(s, q, chunk):
            part = shard(s, q, chunk)
            return copy(("pair", s, chunk), part, part, {"rep": me ^ 1})

        def pass_pair(s, q, chunk):
            part = shard(s, q, chunk)
            return copy(("pass", s, chunk), part, part, {"rep": me ^ 1})

        def parcel(key, pairs, device):
            return [Parcel(keys.setdefault(key, len(keys)), pairs, device)] if pairs else []

        def boxes(name, s, side, n, chunk, pieces, device, start):
            pairs = []
            for a, b, lo, hi in pieces:
                src = wides[s].at[pl.ds(start + a, b - a), pl.ds(lo, hi - lo)]
                dst = wides[s].at[pl.ds(base(side) + a, b - a), pl.ds(lo, hi - lo)]
                pairs.append((src, dst))
            return parcel((name, s, side, n, chunk), pairs, device)

        def group(who, n):
            return who ^ 2 if n else who

        def to_layer(s, side, n, chunk):
            pieces = cut(sent(s, me, side, n), group(me, n), chunk)
            return boxes("x", s, side, n, chunk, pieces, {"layer": after if side == 1 else before}, rows)

        def layer_pass(s, side, n, chunk, who):
            pieces = cut(sent(s, who, side, n), group(who, n), chunk)
            return boxes("xp", s, side, n, chunk, pieces, {"rep": me ^ 1}, base(side))

        def relay(s, chunk, who):
            pieces = cut(shared(who), who, chunk) if s == "u" or who // 2 else []
            side = own_side(who)
            return boxes("r", s, side, 0, chunk, pieces, {"rep": me ^ 2}, base(side))

        def relay_pass(s, chunk, who):
            pieces = cut(shared(who), who, chunk) if s == "u" or who // 2 else []
            side = own_side(who)
            return boxes("rp", s, side, 0, chunk, pieces, {"rep": me ^ 1}, base(side))

        def partial_out(s, chunk):
            source, target = partials[s]
            pairs = []
            for a, b, lo, hi in cut(own_spans(me), me, chunk):
                at = (pl.ds(a, b - a), pl.ds(lo - me * slots, hi - lo))
                pairs.append((source.at[at], target.at[at]))
            return parcel(("p", s, chunk), pairs, {"layer": after if chip == 0 else before})

        def start_swap(s, chunk):
            begin(None, [swap(s, me, chunk)])

        def start_pair(s, chunk):
            begin(None, [pair(s, me, chunk)])

        def end_swap(s, chunk):
            take(None, [swap(s, me ^ 2, chunk)], [pass_pair(s, me ^ 2, chunk)])

        def send_layer(s, n, chunk):
            for side in (1, -1):
                begin(may_send[side], to_layer(s, side, n, chunk))

        def take_layer(s, n, chunk):
            for side in (1, -1):
                take(may_take[side], to_layer(s, side, n, chunk), layer_pass(s, side, n, chunk, me))

        def take_layer_pass(s, n, chunk):
            for side in (1, -1):
                take(may_take[side], layer_pass(s, side, n, chunk, me ^ 1))

        def take_relay(s, chunk):
            take(may_take[own_side(me ^ 2)], relay(s, chunk, me ^ 2), relay_pass(s, chunk, me ^ 2))

        def take_relay_pass(s, chunk):
            take(may_take[own_side(me ^ 2)], relay_pass(s, chunk, me ^ 3))

        out_side = 1 if chip == 0 else -1

        for chunk in chunks:
            start_swap("y", chunk)
        yield
        for s in ("z", "y"):
            for chunk in chunks:
                send_layer(s, 0, chunk)
        for chunk in chunks:
            start_swap("z", chunk)
        for s in ("y", "z"):
            for chunk in chunks:
                start_pair(s, chunk)
        for chunk in chunks:
            end_swap("y", chunk)
            send_layer("y", 1, chunk)
        for chunk in chunks:
            take_layer("z", 0, chunk)
        for chunk in chunks:
            take(None, [pair("y", me ^ 1, chunk)])
            take(None, [pass_pair("y", me ^ 3, chunk)])
            take_layer_pass("z", 0, chunk)
        yield
        for chunk in chunks:
            begin(may_send[out_side], partial_out("c", chunk))
        for n, chunk in enumerate(chunks[:-1]):
            end_swap("z", chunk)
            take_layer("y", 1, chunk)
            take(None, [pair("z", me ^ 1, chunk)])
            if n:
                take(None, [pass_pair("z", me ^ 3, chunks[n - 1])])
                yield
        take_layer("y", 1, chunks[-1])
        for chunk in chunks:
            if chip == 1:
                take_layer("y", 0, chunk)
            take_layer_pass("y", 1, chunk)
        if chip == 1:
            for chunk in chunks:
                take_layer_pass("y", 0, chunk)
        take(None, [pair("z", me ^ 1, chunks[-1])])
        take(None, [pass_pair("z", me ^ 3, chunks[-2])])
        for chunk in chunks:
            if chunk == chunks[1]:
                end_swap("z", chunks[-1])
                for one in chunks:
                    send_layer("z", 1, one)
            if chunk == chunks[-1]:
                take(None, [pass_pair("z", me ^ 3, chunk)])
            if chip == 0:
                take_layer("y", 0, chunk)
                take_layer_pass("y", 0, chunk)
            take(may_take[out_side], partial_out("c", chunk))
            yield
            start_swap("u", chunk)
            start_pair("u", chunk)
            if chunk == chunks[-2]:
                for one in chunks[:-1]:
                    send_layer("u", 0, one)
        send_layer("u", 0, chunks[-1])
        for chunk in chunks:
            begin(may_take[own_side(me)], relay("z", chunk, me))
        first, last = chunks[: len(chunks) // 2], chunks[len(chunks) // 2 :]
        for some in (first, last):
            for chunk in some:
                if chunk != chunks[-1]:
                    end_swap("u", chunk)
                take_layer("u", 0, chunk)
            for chunk in some:
                take_layer_pass("u", 0, chunk)
            yield
        for chunk in chunks:
            begin(may_send[out_side], partial_out("z", chunk))
        for chunk in chunks[:: 1 if chip == 0 else -1]:
            begin(may_take[own_side(me)], relay("u", chunk, me))
        for chunk in chunks:
            if chunk == chunks[-1]:
                end_swap("u", chunk)
            take(None, [pair("u", me ^ 1, chunk)])
            take(None, [pass_pair("u", me ^ 3, chunk)])
        yield
        for chunk in chunks:
            begin(may_send[out_side], partial_out("y", chunk))
        yield
        for chunk in chunks:
            take_relay("z", chunk)
            take_layer("z", 1, chunk)
        yield
        for chunk in chunks:
            take_relay_pass("z", chunk)
            take_layer_pass("z", 1, chunk)
        yield
        arriving = chunks[:: 1 if chip == 1 else -1]
        for chunk in arriving[:2]:
            take_relay("u", chunk)
        for chunk in chunks:
            take(may_take[out_side], partial_out("z", chunk))
        yield
        for n, chunk in enumerate(arriving):
            for one in arriving[n + 1 : n + 2] if n else ():
                take_relay("u", one)
            take_relay_pass("u", chunk)
            yield
        for chunk in chunks:
            take(may_take[out_side], partial_out("y", chunk))
        yield
        for guard, made in remote:

            def end(made=made):
                for one in made:
                    one.wait_send()

            if made:
                end() if guard is None else pl.when(guard)(end)
        yield

    plans = [schedule(me) for me in range(reps)]

    def advance():
        for me in range(reps):
            pl.when(rep == me)(functools.partial(next, plans[me]))

    down = lax.broadcasted_iota(jnp.int32, (tile, tile), 0)
    right_at = lax.broadcasted_iota(jnp.int32, (tile, tile), 1)
    identity = jnp.where(down == right_at, 1.5, 0.0).astype(jnp.float32)
    zero = jnp.zeros((tile, tile), jnp.bfloat16)

    def multiply(lefts, rights):
        wide = jnp.concatenate(lefts, axis=1)
        tall = jnp.concatenate([jnp.concatenate(one, axis=1) for one in rights], axis=0)
        return jnp.dot(wide, tall, preferred_element_type=jnp.float32)

    def own_part(i, left, right):
        lefts, rights = [], []
        for t in range(rows):
            u = half - i + t
            lefts.append(left[rows + i, u])
            line = []
            for w in range(slots):
                v = rep * slots + w + i - t
                good = jnp.logical_and(v >= 0, v < band)
                line.append(jnp.where(good, right[rows + t, lax.rem(v + band, band)], zero))
            rights.append(line)
        return multiply(lefts, rights)

    def halo_part(i, left, right):
        lefts, rights = [], []
        for t in range(rows):
            u = lax.rem(t - i + band, band)
            lefts.append(left[rows + i, u])
            line = []
            row = layer * rows + i - half + u
            inside = jnp.logical_and(row >= 0, row < layers * rows)
            for w in range(slots):
                v = rep * slots + w + half - u
                good = jnp.logical_and(inside, jnp.logical_and(v >= 0, v < band))
                k = i - half + rep * slots + w
                good = jnp.logical_and(good, jnp.logical_and(k >= 0, k < rows))
                line.append(jnp.where(good, right[i + u, lax.rem(v + band, band)], zero))
            rights.append(line)
        return multiply(lefts, rights)

    def split(total, w):
        return total[:, w * tile : (w + 1) * tile]

    def returned(part, i, w):
        k = i - half + rep * slots + w
        below = jnp.logical_and(k < 0, layer > 0)
        above = jnp.logical_and(k >= rows, layer + 1 < layers)
        return jnp.where(jnp.logical_or(below, above), part[i, w].astype(jnp.float32), 0.0)

    def update_rows(chunk):
        def row(i, _):
            total = halo_part(i, z_wide, y_wide)
            for w in range(slots):
                value = -0.5 * (split(total, w) + z_sum[i, w] + returned(c_in, i, w))
                value += jnp.where(rep * slots + w == half, identity, 0.0)
                value = jnp.where(pattern[i, w] == 1, value, 0.0)
                u_wide[rows + i, rep * slots + w] = value.astype(jnp.bfloat16)
            return 0

        lax.fori_loop(chunk[0], chunk[1], row, 0)

    def own_rows(left, right, total, chunk):
        def row(i, _):
            value = own_part(i, left, right)
            for w in range(slots):
                total[i, w] = split(value, w)
            return 0

        lax.fori_loop(chunk[0], chunk[1], row, 0)

    def halo_rows(left, right, total, n, turn):
        def row(r, _):
            i = n * step + r
            if turn:
                i = lax.div(rep, 2) * (2 * n * step + step - rows) + rows - step - n * step + r
            value = halo_part(i, left, right)
            for w in range(slots):
                total[i, w] += split(value, w)
            return 0

        lax.fori_loop(0, step if turn else rows, row, 0)

    def partial_rows(left, right, out, chunk):
        chip = lax.div(rep, 2)

        def row(i, _):
            lefts, rights = [], []
            for t in range(rows):
                u = t + half * chip
                part = left[2 * rows * (1 - chip) + i, u]
                lefts.append(jnp.where(lax.div(i + t, rows) == chip, part, zero))
                j = lax.rem(i + t, rows)
                rights.append([
                    right[rows + j, rep * slots + w + half - u] for w in range(slots)
                ])
            value = multiply(lefts, rights)
            for w in range(slots):
                out[i, w] = split(value, w).astype(jnp.bfloat16)
            return 0

        lax.fori_loop(chunk[0], chunk[1], row, 0)

    def finish(total, part, result):
        def row(i, _):
            for w in range(slots):
                value = jnp.where(pattern[i, w] == 1, total[i, w] + returned(part, i, w), 0.0)
                result[i, w] = value.astype(jnp.bfloat16)
            return 0

        lax.fori_loop(0, rows, row, 0)

    keep(y_own, y_wide)
    pl.semaphore_wait(barrier, 4)
    advance()
    keep(z_own, z_wide)
    middle = rows // 2
    advance()
    partial_rows(z_wide, y_wide, c_out, (0, rows))
    for chunk in chunks[:-2]:
        advance()
        own_rows(z_wide, y_wide, z_sum, chunk)
    for chunk in chunks:
        advance()
        if chunk == chunks[0]:
            own_rows(z_wide, y_wide, z_sum, chunks[-2])
        if chunk == chunks[-1]:
            own_rows(z_wide, y_wide, z_sum, chunk)
        update_rows(chunk)
    for chunk in ((0, middle), (middle, rows)):
        advance()
        partial_rows(u_wide, z_wide, z_out, chunk)
    advance()
    partial_rows(y_wide, u_wide, y_out, (0, rows))
    advance()
    own_rows(u_wide, z_wide, z_sum, (0, rows))
    advance()
    own_rows(y_wide, u_wide, y_sum, (0, rows))
    advance()
    halo_rows(u_wide, z_wide, z_sum, 0, False)
    advance()
    finish(z_sum, z_in, z_next)
    for n in range(len(chunks)):
        advance()
        halo_rows(y_wide, u_wide, y_sum, n, True)
    advance()
    finish(y_sum, y_in, y_next)
    advance()
    assert len(keys) <= recv_sems.shape[0]


def solution(mesh):
    layers, reps = mesh.shape["layer"], mesh.shape["rep"]

    def body(inverse_root, square_root, pattern):
        rows, slots = pattern.shape
        tile = inverse_root.shape[2:]
        local = jax.ShapeDtypeStruct((rows, slots) + tile, jnp.bfloat16)
        wide = pltpu.VMEM((3 * rows, slots * reps) + tile, jnp.bfloat16)
        sems = [pltpu.SemaphoreType.DMA((SEMAPHORES,))] * 2
        paired = reps == 4 and 2 * rows == slots * reps and rows % 4 == 0
        kernel, extra = step_kernel, []
        if paired:
            kernel = paired_kernel
            extra = [pltpu.VMEM((rows, slots) + tile, jnp.float32)] * 2
            extra += [pltpu.VMEM((rows, slots) + tile, jnp.bfloat16)] * 6
            sems = [pltpu.SemaphoreType.DMA((1,)), pltpu.SemaphoreType.DMA((PAIRED_SEMAPHORES,))]
        return pl.pallas_call(
            functools.partial(kernel, layers, reps, (rows, slots, tile[0])),
            out_shape=(local, local),
            in_specs=[SMEM, VMEM, VMEM],
            out_specs=(VMEM, VMEM),
            scratch_shapes=[wide, wide, wide] + extra + sems,
            compiler_params=pltpu.CompilerParams(
                collective_id=0, has_side_effects=True, vmem_limit_bytes=VMEM_BYTES if paired else 60 * 1024 * 1024
            ),
            name="newton_step",
        )(pattern, inverse_root, square_root)

    placed = P("layer", "rep", None, None)
    return jax.shard_map(
        body,
        mesh=mesh,
        in_specs=(placed, placed, P("layer", "rep")),
        out_specs=(placed, placed),
        check_vma=False,
    )
```
